32 devices in a mesh: rep: 2 (over x), dp: 16 (over y, z, core).
Axes of the slice: x: 2, y: 2, z: 4, core: 2. Of those that a mesh axis runs over, the one named last changes fastest.
Arguments:
- x: bfloat16 [32, 2048, 640], P(('rep', 'dp')), parts along dimension 0
- dy: bfloat16 [32, 2048, 640], P(('rep', 'dp')), parts along dimension 0
- w_gate: bfloat16 [2, 640, 2560], replicated
- w_up: bfloat16 [2, 640, 2560], replicated
- w_down: bfloat16 [2, 2560, 640], replicated
- m_w_gate: float32 [2, 640, 2560], P(None, 'dp')
- m_w_up: float32 [2, 640, 2560], P(None, 'dp')
- m_w_down: float32 [2, 2560, 640], P(None, 'dp')
- v_w_gate: float32 [2, 640, 2560], P(None, 'dp')
- v_w_up: float32 [2, 640, 2560], P(None, 'dp')
- v_w_down: float32 [2, 2560, 640], P(None, 'dp')
Outputs:
- output 1: bfloat16 [4, 640, 2560], P('rep'), parts along dimension 0
- output 2: bfloat16 [4, 640, 2560], P('rep'), parts along dimension 0
- output 3: bfloat16 [4, 2560, 640], P('rep'), parts along dimension 0
- output 4: float32 [4, 640, 2560], P('rep', 'dp'), parts along dimension 0
- output 5: float32 [4, 640, 2560], P('rep', 'dp'), parts along dimension 0
- output 6: float32 [4, 2560, 640], P('rep', 'dp'), parts along dimension 0
- output 7: float32 [4, 640, 2560], P('rep', 'dp'), parts along dimension 0
- output 8: float32 [4, 640, 2560], P('rep', 'dp'), parts along dimension 0
- output 9: float32 [4, 2560, 640], P('rep', 'dp'), parts along dimension 0
There are 2 independent parts. The reference program is written for one: setup_inputs(seed, part) draws one part's arguments, and reference() takes and returns one part's arrays. A program takes and returns all parts, laid end to end along the dimension named above; an argument that names none is the same for every part.
All inputs are finite; a program needn't handle non-finite values.
Results may differ from the reference program's by a relative error of at most 0.022.
Values are sent between devices in bfloat16 or wider.
A program may use at most 2 GiB of HBM per device.

```python
import jax
import jax.numpy as jnp
from jax import lax

SEQUENCES = 16
TOKENS = 2048
D = 640
FF = 2560
LAYERS = 2
NAMES = ("w_gate", "w_up", "w_down")
SHAPES = {"w_gate": (LAYERS, D, FF), "w_up": (LAYERS, D, FF), "w_down": (LAYERS, FF, D)}


def bump(key, n, height):
    away = (jnp.arange(n, dtype=jnp.int32) - jax.random.randint(key, (), 0, n, jnp.int32)) % n
    return jnp.where(away < n // 8, height, 1.0)


def together(key, own, strength):
    shared = jax.random.normal(key, own.shape[1:], jnp.float32)
    return (own + strength * shared) * lax.rsqrt(1 + strength * strength)


def setup_inputs(seed: int = 0, part: int = 0) -> dict:
    kx, kdy, ka, kb, kz, kf, kh, kl, *keys = jax.random.split(jax.random.key(seed), 8 + 3 * len(NAMES))
    kx, kdy, ka, kb = (jax.random.fold_in(k, part) for k in (kx, kdy, ka, kb))
    kw, km, kv = (keys[i::3] for i in range(3))
    shape = (SEQUENCES, TOKENS, D)
    much_x, much_dy = jax.random.uniform(kz, (2,), jnp.float32, 0.0, 1.0)
    loud = 2.0 ** jax.random.uniform(jax.random.fold_in(kz, 1), (), jnp.float32, -1.0, 2.0)
    layers = 2.0 ** jax.random.uniform(kl, (LAYERS, 1, 1), jnp.float32, -1.0, 1.0)
    x = together(ka, jax.random.normal(kx, shape, jnp.float32), much_x) * bump(kf, D, 4.0)
    dy = together(kb, jax.random.normal(kdy, shape, jnp.float32), much_dy)
    drawn = {"x": x.astype(jnp.bfloat16), "dy": (loud * dy * (SEQUENCES * TOKENS) ** -0.5).astype(jnp.bfloat16)}
    for key, name in zip(kw, NAMES, strict=True):
        w = jax.random.normal(key, SHAPES[name], jnp.float32) * SHAPES[name][1] ** -0.5
        drawn[name] = (w * {"w_gate": 1.0, "w_up": bump(kh, FF, 4.0), "w_down": layers}[name]).astype(jnp.bfloat16)
    for key, name in zip(km, NAMES, strict=True):
        drawn[f"m_{name}"] = 0.1 * jax.random.normal(key, SHAPES[name], jnp.float32)
    for key, name in zip(kv, NAMES, strict=True):
        drawn[f"v_{name}"] = jax.random.uniform(key, SHAPES[name], jnp.float32, 0.005, 0.015)
    return drawn


def matmul(a, w):
    return jnp.dot(a, w, preferred_element_type=jnp.float32).astype(jnp.bfloat16)


def normed(h):
    wide = h.astype(jnp.float32)
    scale = lax.rsqrt(jnp.mean(wide**2, -1, keepdims=True) + 1e-6)
    return (wide * scale).astype(jnp.bfloat16)


def layer(h, w):
    a = normed(h)
    gate = jnp.dot(a, w["w_gate"], preferred_element_type=jnp.float32)
    up = jnp.dot(a, w["w_up"], preferred_element_type=jnp.float32)
    return h + matmul((jax.nn.silu(gate) * up).astype(jnp.bfloat16), w["w_down"])


def adamw(w, m, v, g):
    m = 0.9 * m + 0.1 * g
    v = 0.95 * v + 0.05 * g * g
    step = m * lax.rsqrt(v + 1e-8) + 0.1 * w
    return (w - 0.02 * step).astype(jnp.bfloat16), m, v


def stack(weights, h):
    return lax.scan(lambda h, w: (layer(h, w), None), h, weights)[0]


def reference(x, dy, w_gate, w_up, w_down, m_w_gate, m_w_up, m_w_down, v_w_gate, v_w_up, v_w_down):
    weights = dict(zip(NAMES, (w_gate, w_up, w_down), strict=True))

    def take(so_far, sequence):
        h, by_y = sequence
        _, back = jax.vjp(lambda w: stack(w, h), weights)
        return jax.tree.map(lambda total, term: total + term.astype(jnp.float32), so_far, back(by_y)[0]), None

    none_yet = {name: jnp.zeros(w.shape, jnp.float32) for name, w in weights.items()}
    by_weights, _ = lax.scan(take, none_yet, (x, dy))
    gradients = [by_weights[name].astype(jnp.bfloat16).astype(jnp.float32) for name in NAMES]
    new = [
        adamw(w.astype(jnp.float32), m, v, g)
        for w, m, v, g in zip((w_gate, w_up, w_down), (m_w_gate, m_w_up, m_w_down), (v_w_gate, v_w_up, v_w_down), gradients, strict=True)
    ]
    return tuple(one[which] for which in range(3) for one in new)
```

```python
import jax
import jax.numpy as jnp
from jax import lax
from jax.experimental import pallas as pl
from jax.experimental.pallas import tpu as pltpu
from jax.sharding import PartitionSpec as P

F32, BF16 = jnp.float32, jnp.bfloat16
NT = (((1,), (1,)), ((), ()))


def dot(a, b):
    return jnp.dot(a, b, preferred_element_type=F32)


def dot_t(a, b):
    return lax.dot_general(a, b, NT, preferred_element_type=F32)


def sigmoid(x):
    return 0.5 * jnp.tanh(0.5 * x) + 0.5


def norm_scale(h):
    wide = h.astype(F32)
    return wide, lax.rsqrt(jnp.mean(wide * wide, -1, keepdims=True) + 1e-6)


def chain_kernel(x_ref, dy_ref, wg_hbm, wu_hbm, wd_hbm, act2_ref, dg2_ref, du2_ref, act1_ref, dg1_ref, du1_ref, at1_ref, at2_ref, dyt_ref, dht_ref,
                 wg, wu, wd, gate1, up1, sems, *, ft):
    ff = wg.shape[2]
    i = pl.program_id(0)
    copies = [pltpu.make_async_copy(src.at[l], dst.at[l], sems.at[l, k]) for l in range(2) for k, (src, dst) in enumerate(((wg_hbm, wg), (wu_hbm, wu), (wd_hbm, wd)))]

    @pl.when(i == 0)
    def _():
        for c in copies:
            c.start()

    def arrived(n):
        @pl.when(i == 0)
        def _():
            copies[n].wait()

    x = x_ref[...]
    dy = dy_ref[...]
    wide, s = norm_scale(x)
    a = (wide * s).astype(BF16)
    at1_ref[...] = a.T
    dyt_ref[...] = dy.T
    arrived(0)
    arrived(1)
    arrived(2)
    total = jnp.zeros(x.shape, F32)
    for f in range(0, ff, ft):
        fs = pl.ds(f, ft)
        gate = dot(a, wg[0, :, fs])
        up = dot(a, wu[0, :, fs])
        gate1[:, fs] = gate
        up1[:, fs] = up
        act = (gate * sigmoid(gate) * up).astype(BF16)
        act1_ref[:, fs] = act
        total += dot(act, wd[0, fs, :])
    h = x + total.astype(BF16)
    arrived(3)
    arrived(4)
    arrived(5)
    wide, s = norm_scale(h)
    a = (wide * s).astype(BF16)
    at2_ref[...] = a.T
    dag = jnp.zeros(x.shape, F32)
    dau = jnp.zeros(x.shape, F32)

    def back(dout, gate, up, l, fs, refs):
        dact = dot_t(dout, wd[l, fs, :]).astype(BF16).astype(F32)
        sig = sigmoid(gate)
        silu = gate * sig
        du = (dact * silu).astype(BF16)
        dg = (dact * up * (sig + silu * (1.0 - sig))).astype(BF16)
        refs[0][:, fs] = dg
        refs[1][:, fs] = du
        return dg, du, silu

    for f in range(0, ff, ft):
        fs = pl.ds(f, ft)
        gate = dot(a, wg[1, :, fs])
        up = dot(a, wu[1, :, fs])
        dg, du, silu = back(dy, gate, up, 1, fs, (dg2_ref, du2_ref))
        act2_ref[:, fs] = (silu * up).astype(BF16)
        dag += dot_t(dg, wg[1, :, fs])
        dau += dot_t(du, wu[1, :, fs])
    da = (dag.astype(BF16) + dau.astype(BF16)).astype(F32)
    inner = jnp.mean(da * wide, -1, keepdims=True)
    dh = dy + (da * s - wide * (s * s * s * inner)).astype(BF16)
    dht_ref[...] = dh.T
    for f in range(0, ff, ft):
        fs = pl.ds(f, ft)
        back(dh, gate1[:, fs], up1[:, fs], 0, fs, (dg1_ref, du1_ref))


def chain(x, dy, wg, wu, wd, tile=256, ft=1280):
    tokens, d = x.shape
    ff = wg.shape[2]
    rows = pl.BlockSpec((tile, d), lambda i: (i, 0))
    cols = pl.BlockSpec((d, tile), lambda i: (0, i))
    wide = pl.BlockSpec((tile, ff), lambda i: (i, 0))
    hbm = pl.BlockSpec(memory_space=pl.ANY)
    return pl.pallas_call(
        lambda *r: chain_kernel(*r, ft=ft),
        grid=(tokens // tile,),
        in_specs=[rows, rows, hbm, hbm, hbm],
        out_specs=[wide] * 6 + [cols] * 4,
        out_shape=[jax.ShapeDtypeStruct((tokens, ff), BF16)] * 6 + [jax.ShapeDtypeStruct((d, tokens), BF16)] * 4,
        scratch_shapes=[pltpu.VMEM(wg.shape, BF16), pltpu.VMEM(wu.shape, BF16), pltpu.VMEM(wd.shape, BF16), pltpu.VMEM((tile, ff), F32), pltpu.VMEM((tile, ff), F32), pltpu.SemaphoreType.DMA((2, 3))],
        compiler_params=pltpu.CompilerParams(dimension_semantics=("arbitrary",), vmem_limit_bytes=63 * 2**20),
        cost_estimate=pl.CostEstimate(flops=9 * 2 * tokens * d * ff, bytes_accessed=100 * 2**20, transcendentals=0),
    )(x, dy, wg, wu, wd)
MESH = pl.DeviceIdType.MESH
CHUNKS = (("down", 1), ("gate", 1), ("up", 1), ("down", 0), ("gate", 0), ("up", 0))
FT = 512
PERIOD, STEP, TILE = 25.0, 5.0, 1.7


def adamw(w, m, v, g):
    m = 0.9 * m + 0.1 * g
    v = 0.95 * v + 0.05 * g * g
    step = m * lax.rsqrt(v + 1e-8) + 0.1 * w
    return (w - 0.02 * step).astype(BF16), m, v


class Chunk:
    def __init__(self, place, bufs, own, ssem, rsem, free):
        self.__dict__.update(place)
        (self.T, self.D, self.YA, self.EA, self.FA, self.EB, self.FB, self.YB) = bufs
        self.w, self.m, self.v = own
        self.ssem, self.rsem, self.free = ssem, rsem, free
        self.R = self.T.shape[3]
        self.RA = self.R * 3 // 5
        self.A, self.B = pl.ds(0, self.RA), pl.ds(self.RA, self.R - self.RA)
        self.sent = []

    def copy(self, src, dst, s, r, dev):
        return pltpu.make_async_remote_copy(src_ref=src, dst_ref=dst, send_sem=self.ssem.at[s], recv_sem=self.rsem.at[r], device_id=dev, device_id_type=MESH)

    def send(self, cond, src, dst, s, r, dev):
        base, o = s if isinstance(s, tuple) else (s, None)
        self.copy(src, dst, base if o is None else base + o, r, dev).start()
        self.sent.append((cond, src.shape, base, o))

    def wait_sent(self):
        R, RA = self.R, self.RA
        like = {
            (2, 4, R): lambda: self.D,
            (RA,): lambda: self.YA.at[0],
            (R - RA,): lambda: self.YB,
            (2, R - RA): lambda: self.EB.at[0],
        }
        for cond, shape, base, o in self.sent[1:]:
            def wait():
                ref = like[tuple(shape[:-1])]()
                self.copy(ref, ref, base if o is None else base + o, 0, self.partner).wait_send()

            self.when(cond, wait)

    def got(self, dst, r):
        self.copy(dst, dst, 0, r, self.partner).wait_recv()

    def when(self, cond, f):
        if cond is None:
            f()
        else:
            pl.when(cond)(f)

    def add(self, dst, *srcs):
        dst[...] = sum(s[...].astype(F32) for s in (dst, *srcs)).astype(BF16)

    def own_y(self, o, rows):
        return self.T.at[self.y, o, self.c, rows, :]

    def both(self, o):
        return self.T.at[:, o, self.c, self.B, :]

    def s0(self):
        self.send(None, self.T.at[:, :, 1 - self.c], self.D, 0, 0, self.partner)

    def s1(self):
        self.got(self.D, 0)
        for n, o in enumerate((self.e1, self.i1, self.i0, self.e0)):
            t = self.D.at[1 - self.y, o, self.A, :]
            self.add(t, self.T.at[1 - self.y, o, self.c, self.A, :])
            self.send(None, t, self.YA.at[o], (1, o), 1 + o, self.across)

        def end():
            for slot, o in enumerate((self.e1, self.i1, self.i0)):
                t = self.D.at[:, o, self.B, :]
                self.add(t, self.both(o))
                self.send(self.end, t, self.EB.at[slot], 11 + slot, 11 + slot, self.inner)

        self.when(self.end, end)

    def s2(self):
        self.copy(self.D, self.D, 0, 0, self.partner).wait_send()
        pl.semaphore_signal(self.free, inc=1, device_id=self.partner, device_id_type=MESH)

        def mid():
            for slot, o in enumerate((self.e1, self.i1)):
                self.got(self.EB.at[slot], 11 + slot)
                t = self.D.at[:, o, self.B, :]
                self.add(t, self.both(o), self.EB.at[slot])
                self.send(self.mid, t, self.FB.at[slot], 14 + slot, 14 + slot, self.inner)

        self.when(self.mid, mid)

    def got_y(self, o):
        self.got(self.YA.at[o], 1 + o)

    def s3(self):
        def end():
            for slot, o in enumerate((self.e1, self.i1, self.i0)):
                self.got_y(o)
                t = self.YA.at[o]
                self.add(t, self.own_y(o, self.A), self.D.at[self.y, o, self.A, :])
                self.send(self.end, t, self.EA.at[slot], 5 + slot, 5 + slot, self.inner)

        def mid():
            self.got(self.FB.at[0], 14)
            t = self.D.at[:, self.e0, self.B, :]
            self.add(t, self.both(self.e0), self.FB.at[0])
            self.send(self.mid, t, self.FB.at[1], 16, 16, self.outer)

        self.when(self.end, end)
        self.when(self.mid, mid)

    def s4(self):
        def mid():
            for slot, o in enumerate((self.e1, self.i1)):
                self.got(self.EA.at[slot], 5 + slot)
                self.got_y(o)
                t = self.YA.at[o]
                self.add(t, self.own_y(o, self.A), self.D.at[self.y, o, self.A, :], self.EA.at[slot])
                self.send(self.mid, t, self.FA.at[slot], 8 + slot, 8 + slot, self.inner)

        self.when(self.mid, mid)
        own = self.T.at[1 - self.y, self.z, self.c, self.B, :]
        d = self.D.at[1 - self.y, self.z, self.B, :]
        t = self.FB.at[1, 1 - self.y]

        def mid2():
            self.got(self.FB.at[1], 15)
            self.got(self.EB.at[2], 13)
            self.add(t, own, d, self.EB.at[2, 1 - self.y])

        def end2():
            self.got(self.FB.at[1], 16)
            self.add(t, own, d)

        self.when(self.mid, mid2)
        self.when(self.end, end2)
        self.send(None, t, self.YB, 17, 17, self.across)

    def step(self, rows, *srcs):
        t = self.own_y(self.z, rows)
        g = sum(s[...].astype(F32) for s in (t, *srcs)).astype(BF16).astype(F32)
        w, m, v = adamw(self.w[rows, :].astype(F32), self.m[rows, :], self.v[rows, :], g)
        t[...] = w
        self.m[rows, :] = m
        self.v[rows, :] = v

    def s5(self):
        def mid():
            self.got(self.FA.at[0], 8)
            self.got_y(self.e0)
            t = self.YA.at[self.e0]
            self.add(t, self.own_y(self.e0, self.A), self.D.at[self.y, self.e0, self.A, :], self.FA.at[0])
            self.send(self.mid, t, self.FA.at[1], 10, 10, self.outer)

        self.when(self.mid, mid)
        self.got(self.YB, 17)
        d = self.D.at[self.y, self.z, self.B, :]
        self.when(self.mid, lambda: self.step(self.B, d, self.YB, self.FB.at[1, self.y], self.EB.at[2, self.y]))
        self.when(self.end, lambda: self.step(self.B, d, self.YB, self.FB.at[1, self.y]))
        t = self.own_y(self.z, self.B)
        self.send(None, t, t, 30, 30, self.across)

    def s6(self):
        self.got_y(self.z)
        d = self.D.at[self.y, self.z, self.A, :]

        def mid():
            self.got(self.FA.at[1], 9)
            self.got(self.EA.at[2], 7)
            self.step(self.A, d, self.YA.at[self.z], self.FA.at[1], self.EA.at[2])

        def end():
            self.got(self.FA.at[1], 10)
            self.step(self.A, d, self.YA.at[self.z], self.FA.at[1])

        self.when(self.mid, mid)
        self.when(self.end, end)
        self.give_a(self.z, None, self.mid, None)
        self.got(self.T.at[1 - self.y, self.z, self.c, self.B, :], 30)
        self.give_b(self.z, None, self.mid)

    def give_a(self, o, inward, outward, cond):
        t = self.own_y(o, self.A)
        if inward is not False:
            self.when(inward, lambda: self.send(inward, t, t, (18, o), 18 + o, self.inner))
        if outward is not False:
            self.when(outward, lambda: self.send(outward, t, t, (22, o), 18 + o, self.outer))
        self.send(cond, t, t, (26, o), 26 + o, self.across)

    def give_b(self, o, inward, outward):
        t = self.both(o)
        if inward is not False:
            self.when(inward, lambda: self.send(inward, t, t, (31, o), 31 + o, self.inner))
        if outward is not False:
            self.when(outward, lambda: self.send(outward, t, t, (35, o), 31 + o, self.outer))

    def got_a(self, o):
        self.got(self.own_y(o, self.A), 18 + o)

    def got_b(self, o):
        self.got(self.both(o), 31 + o)

    def plain(self, cond, o, inward, outward, which):
        if which == "a":
            t = self.own_y(o, self.A)
            self.got_a(o)
            base = 18
        else:
            t = self.both(o)
            self.got_b(o)
            base = 31
        if inward:
            self.send(cond, t, t, (base, o), base + o, self.inner)
        if outward:
            self.send(cond, t, t, (base + 4, o), base + o, self.outer)
        if which == "a":
            self.send(cond, t, t, (26, o), 26 + o, self.across)

    def g1(self, which):
        def mid():
            self.plain(self.mid, self.e0, True, False, which)
            self.plain(self.mid, self.i1, False, True, which)

        self.when(self.mid, mid)
        self.when(self.end, lambda: self.plain(self.end, self.i0, False, False, which))

    def g2(self, which):
        self.when(self.mid, lambda: self.plain(self.mid, self.e1, False, True, which))
        self.when(self.end, lambda: self.plain(self.end, self.i1, False, False, which))

    def g3(self, which):
        self.when(self.end, lambda: self.plain(self.end, self.e1, False, False, which))

    def s7(self):
        self.g1("a")

    def s8(self):
        self.g1("b")
        self.g2("a")

    def s9(self):
        self.g2("b")
        self.g3("a")

    def s10(self):
        self.g3("b")
        for o in range(4):
            self.got(self.T.at[1 - self.y, o, self.c, self.A, :], 26 + o)
        pl.semaphore_wait(self.free, 1)
        t = self.T.at[:, :, self.c]
        self.send(None, t, t, 39, 39, self.partner)

    def s11(self):
        self.got(self.T.at[:, :, 1 - self.c], 39)
        self.wait_sent()

    STEPS = ("s0", "s1", "s2", "s3", "s4", "s5", "s6", "s7", "s8", "s9", "s10", "s11")


def kernel(act2, dg2, du2, act1, dg1, du1, at1, at2, dyt, dht, wg, wu, wd, mg, mu, md, vg, vu, vd,
           o_wg, o_wu, o_wd, o_mg, o_mu, o_md, o_vg, o_vu, o_vd,
           tg, tu, td, dG, dDn, yaG, yaD, eaG, eaD, faG, faD, ebG, ebD, fbG, fbD, ybG, ybD,
           lhs, rhs, sw_g, sw_u, sw_d, sm_g, sm_u, sm_d, sv_g, sv_u, sv_d,
           ssem, rsem, lsem, tsem, isem, osem, free):
    rep, me = lax.axis_index("rep"), lax.axis_index("dp")
    c, z, y = me % 2, (me // 2) % 4, me // 8

    def dev(y, z, c):
        return (rep, y * 8 + z * 2 + c)

    low = z < 2
    e0, i0, i1, e1 = (jnp.where(low, p, 3 - p) for p in range(4))
    end = (z == 0) | (z == 3)
    mid = (z == 1) | (z == 2)
    inner = dev(y, jnp.where(end, i0, i1), c)
    outer = dev(y, e0, c)
    place = dict(y=y, z=z, c=c, e0=e0, i0=i0, i1=i1, e1=e1, end=end, mid=mid, inner=inner, outer=outer, across=dev(1 - y, z, c), partner=dev(y, z, 1 - c))

    owns = {"gate": (sw_g, sm_g, sv_g), "up": (sw_u, sm_u, sv_u), "down": (sw_d, sm_d, sv_d)}
    T = {"gate": tg, "up": tu, "down": td}
    loads, stores = [], []
    for n, (name, hw, hm, hv, ow, om, ov) in enumerate((("gate", wg, mg, vg, o_wg, o_mg, o_vg), ("up", wu, mu, vu, o_wu, o_mu, o_vu), ("down", wd, md, vd, o_wd, o_md, o_vd))):
        sw, sm, sv = owns[name]
        loads += [pltpu.make_async_copy(hw.at[:, me], sw, isem.at[n, 0]), pltpu.make_async_copy(hm, sm, isem.at[n, 1]), pltpu.make_async_copy(hv, sv, isem.at[n, 2])]
    outs = {"gate": (o_wg, o_mg, o_vg), "up": (o_wu, o_mu, o_vu), "down": (o_wd, o_md, o_vd)}

    left = {("down", 1): dyt, ("gate", 1): at2, ("up", 1): at2, ("down", 0): dht, ("gate", 0): at1, ("up", 0): at1}
    right = {("down", 1): act2, ("gate", 1): dg2, ("up", 1): du2, ("down", 0): act1, ("gate", 0): dg1, ("up", 0): du1}
    tiles = right[CHUNKS[0]].shape[1] // FT

    def rhs_copy(k, j):
        t = tiles * k + j
        return pltpu.make_async_copy(right[CHUNKS[k]].at[:, pl.ds(j * FT, FT)], rhs.at[t % 2], tsem.at[t % 2])

    def lhs_copy(k):
        s = 0 if CHUNKS[k][0] == "down" else 1
        return pltpu.make_async_copy(left[CHUNKS[k]], lhs.at[s], lsem.at[s])

    lhs_copy(0).start()
    rhs_copy(0, 0).start()
    lhs_copy(1).start()

    barrier = pltpu.get_barrier_semaphore()
    for d, cond in ((place["partner"], None), (place["across"], None), (inner, None), (outer, mid)):
        if cond is None:
            pl.semaphore_signal(barrier, inc=1, device_id=d, device_id_type=MESH)
        else:
            @pl.when(cond)
            def _():
                pl.semaphore_signal(barrier, inc=1, device_id=d, device_id_type=MESH)
    pl.when(mid)(lambda: pl.semaphore_wait(barrier, 4))
    pl.when(end)(lambda: pl.semaphore_wait(barrier, 3))

    chunks = []
    counts = {"gate": 0, "down": 0}
    for k, (name, l) in enumerate(CHUNKS):
        kind = "down" if name == "down" else "gate"
        n = counts[kind]
        counts[kind] += 1
        pick = 1 if kind == "down" else 0
        bufs = [T[name].at[l]] + [b[pick].at[n] for b in ((dG, dDn), (yaG, yaD), (eaG, eaD), (faG, faD), (ebG, ebD), (fbG, fbD), (ybG, ybD))]
        chunks.append(Chunk(place, bufs, [b.at[l] for b in owns[name]], ssem.at[k], rsem.at[k], free.at[k]))

    def finish(k):
        name, l = CHUNKS[k]
        for i, (src, dst) in enumerate(zip((T[name],) + owns[name][1:], outs[name])):
            cp = pltpu.make_async_copy(src.at[l], dst.at[l], osem.at[k, i])
            cp.start()
            stores.append(cp)

    started = set()

    def run(k, s):
        if (k, s) == (0, 5):
            for cp in loads:
                cp.wait()
        getattr(chunks[k], Chunk.STEPS[s])()
        if s == len(Chunk.STEPS) - 1:
            finish(k)

    plan = sorted((max(tiles * (k + 1), tiles + (PERIOD * k + STEP * s) / TILE), s * -1, k, s) for k in range(len(CHUNKS)) for s in range(len(Chunk.STEPS)))
    total_tiles = tiles * len(CHUNKS)
    slots = {}
    for at, _, k, s in plan:
        slots.setdefault(min(int(at), total_tiles), []).append((k, s))
    for v in slots.values():
        pass

    for k, (name, l) in enumerate(CHUNKS):
        if k == 0:
            for cp in loads:
                cp.start()
        if k in (0, 1, 3, 4):
            lhs_copy(k).wait()
        side = 0 if name == "down" else 1

        def tile(j, _, k=k, name=name, l=l, side=side):
            t = tiles * k + j
            rhs_copy(k, j).wait()

            @pl.when(j < tiles - 1)
            def _():
                rhs_copy(k, j + 1).start()

            if k + 1 < len(CHUNKS):
                @pl.when(j == tiles - 1)
                def _():
                    rhs_copy(k + 1, 0).start()

            out = jnp.dot(lhs[side], rhs[t % 2], preferred_element_type=F32).astype(BF16)
            if name == "down":
                out = out.T
                for q in range(FT // 32):
                    n = (FT // 32) * j + q
                    b, r = n // 5, pl.multiple_of((n % 5) * 32, 32)
                    td[l, b // 8, (b // 2) % 4, b % 2, pl.ds(r, 32), :] = out[32 * q : 32 * q + 32]
            else:
                T[name][l, :, :, :, :, pl.ds(pl.multiple_of(j * FT, FT), FT)] = out.reshape(2, 4, 2, 40, FT)
            for jj in range(tiles):
                todo = slots.get(tiles * k + jj, [])
                if todo:
                    @pl.when(j == jj)
                    def _(todo=todo):
                        for kk, s in todo:
                            run(kk, s)
            return 0

        lax.fori_loop(0, tiles, tile, 0)
        if k == 0:
            lhs_copy(3).start()
        if k == 2:
            lhs_copy(4).start()
    for kk, s in slots.get(total_tiles, []):
        run(kk, s)
    for cp in stores:
        cp.wait()


def comm(parts, weights, moments, ):
    hbm = pl.BlockSpec(memory_space=pl.ANY)
    wg, wu, wd = weights
    blocks = [w.reshape(w.shape[0], 16, w.shape[1] // 16, w.shape[2]) for w in weights]
    outs = [jax.ShapeDtypeStruct((2, 2, 4, 2) + b.shape[2:], BF16) for b in blocks]
    outs += [jax.ShapeDtypeStruct(t.shape, F32) for t in moments]
    g, d = (40, 2560), (160, 640)

    def pair(*lead, a=None):
        def rows(s):
            return {None: s[0], "A": s[0] * 3 // 5, "B": s[0] * 2 // 5}[a]
        return [pltpu.VMEM((4, *lead, rows(g), g[1]), BF16), pltpu.VMEM((2, *lead, rows(d), d[1]), BF16)]

    scratch = [pltpu.VMEM((2, 2, 4, 2) + b.shape[2:], BF16) for b in blocks]
    scratch += pair(2, 4) + pair(4, a="A") + pair(3, a="A") + pair(2, a="A") + pair(3, 2, a="B") + pair(2, 2, a="B") + pair(a="B")
    scratch += [pltpu.VMEM((2, 640, 2048), BF16), pltpu.VMEM((2, 2048, FT), BF16)]
    scratch += [pltpu.VMEM((2,) + b.shape[2:], BF16) for b in blocks]
    scratch += [pltpu.VMEM((2,) + b.shape[2:], F32) for b in blocks] * 2
    dma = pltpu.SemaphoreType.DMA
    scratch += [dma((6, 40)), dma((6, 40)), dma((2,)), dma((2,)), dma((3, 3)), dma((6, 3)), pltpu.SemaphoreType.REGULAR((6,))]
    return pl.pallas_call(
        kernel,
        in_specs=[hbm] * 19,
        out_specs=[hbm] * 9,
        out_shape=outs,
        scratch_shapes=scratch,
        compiler_params=pltpu.CompilerParams(collective_id=0, has_side_effects=True, vmem_limit_bytes=67043328),
        cost_estimate=pl.CostEstimate(flops=6 * 2 * 2048 * 640 * 2560, bytes_accessed=100 * 2**20, transcendentals=0),
    )(*parts, *blocks, *moments)


def solution(mesh):
    def step(x, dy, wg, wu, wd, *moments):
        parts = chain(x[0], dy[0], wg, wu, wd)
        new = comm(parts, (wg, wu, wd), moments)
        return tuple(t.reshape(w.shape) for t, w in zip(new, (wg, wu, wd))) + tuple(new[3:])

    whole, rows = P(None, None, None), P(None, "dp", None)
    return jax.shard_map(
        step,
        mesh=mesh,
        in_specs=(P(("rep", "dp")),) * 2 + (whole,) * 3 + (rows,) * 6,
        out_specs=(P("rep", None, None),) * 3 + (P("rep", "dp", None),) * 6,
        check_vma=False,
    )
```

```python
import jax
import jax.numpy as jnp
from jax import lax
from jax.experimental import pallas as pl
from jax.experimental.pallas import tpu as pltpu
from jax.sharding import PartitionSpec as P

F32, BF16 = jnp.float32, jnp.bfloat16
NT = (((1,), (1,)), ((), ()))


def dot(a, b):
    return jnp.dot(a, b, preferred_element_type=F32)


def dot_t(a, b):
    return lax.dot_general(a, b, NT, preferred_element_type=F32)


def sigmoid(x):
    return 0.5 * jnp.tanh(0.5 * x) + 0.5


def norm_scale(h):
    wide = h.astype(F32)
    return wide, lax.rsqrt(jnp.mean(wide * wide, -1, keepdims=True) + 1e-6)


def chain_kernel(x_ref, dy_ref, wg_hbm, wu_hbm, wd_hbm, act2_ref, dg2_ref, du2_ref, act1_ref, dg1_ref, du1_ref, at1_ref, at2_ref, dyt_ref, dht_ref,
                 wg, wu, wd, gate1, up1, sems, *, ft):
    ff = wg.shape[2]
    i = pl.program_id(0)
    copies = [pltpu.make_async_copy(src.at[l], dst.at[l], sems.at[l, k]) for l in range(2) for k, (src, dst) in enumerate(((wg_hbm, wg), (wu_hbm, wu), (wd_hbm, wd)))]

    @pl.when(i == 0)
    def _():
        for c in copies:
            c.start()

    def arrived(n):
        @pl.when(i == 0)
        def _():
            copies[n].wait()

    x = x_ref[...]
    dy = dy_ref[...]
    wide, s = norm_scale(x)
    a = (wide * s).astype(BF16)
    at1_ref[...] = a.T
    dyt_ref[...] = dy.T
    arrived(0)
    arrived(1)
    total = jnp.zeros(x.shape, F32)
    for f in range(0, ff, ft):
        fs = pl.ds(f, ft)
        gate = dot(a, wg[0, :, fs])
        up = dot(a, wu[0, :, fs])
        gate1[:, fs] = gate
        up1[:, fs] = up
        act = (gate * sigmoid(gate) * up).astype(BF16)
        act1_ref[:, fs] = act
        if f == 0:
            arrived(2)
        total += dot(act, wd[0, fs, :])
    h = x + total.astype(BF16)
    arrived(3)
    arrived(4)
    arrived(5)
    wide, s = norm_scale(h)
    a = (wide * s).astype(BF16)
    at2_ref[...] = a.T
    dag = jnp.zeros(x.shape, F32)
    dau = jnp.zeros(x.shape, F32)

    def back(dout, gate, up, l, fs, refs):
        dact = dot_t(dout, wd[l, fs, :]).astype(BF16).astype(F32)
        sig = sigmoid(gate)
        silu = gate * sig
        du = (dact * silu).astype(BF16)
        dg = (dact * up * (sig + silu * (1.0 - sig))).astype(BF16)
        refs[0][:, fs] = dg
        refs[1][:, fs] = du
        return dg, du, silu

    for f in range(0, ff, ft):
        fs = pl.ds(f, ft)
        gate = dot(a, wg[1, :, fs])
        up = dot(a, wu[1, :, fs])
        dg, du, silu = back(dy, gate, up, 1, fs, (dg2_ref, du2_ref))
        act2_ref[:, fs] = (silu * up).astype(BF16)
        dag += dot_t(dg, wg[1, :, fs])
        dau += dot_t(du, wu[1, :, fs])
    da = (dag.astype(BF16) + dau.astype(BF16)).astype(F32)
    inner = jnp.mean(da * wide, -1, keepdims=True)
    dh = dy + (da * s - wide * (s * s * s * inner)).astype(BF16)
    dht_ref[...] = dh.T
    for f in range(0, ff, ft):
        fs = pl.ds(f, ft)
        back(dh, gate1[:, fs], up1[:, fs], 0, fs, (dg1_ref, du1_ref))


def chain(x, dy, wg, wu, wd, tile=256, ft=1280):
    tokens, d = x.shape
    ff = wg.shape[2]
    rows = pl.BlockSpec((tile, d), lambda i: (i, 0))
    cols = pl.BlockSpec((d, tile), lambda i: (0, i))
    wide = pl.BlockSpec((tile, ff), lambda i: (i, 0))
    hbm = pl.BlockSpec(memory_space=pl.ANY)
    return pl.pallas_call(
        lambda *r: chain_kernel(*r, ft=ft),
        grid=(tokens // tile,),
        in_specs=[rows, rows, hbm, hbm, hbm],
        out_specs=[wide] * 6 + [cols] * 4,
        out_shape=[jax.ShapeDtypeStruct((tokens, ff), BF16)] * 6 + [jax.ShapeDtypeStruct((d, tokens), BF16)] * 4,
        scratch_shapes=[pltpu.VMEM(wg.shape, BF16), pltpu.VMEM(wu.shape, BF16), pltpu.VMEM(wd.shape, BF16), pltpu.VMEM((tile, ff), F32), pltpu.VMEM((tile, ff), F32), pltpu.SemaphoreType.DMA((2, 3))],
        compiler_params=pltpu.CompilerParams(dimension_semantics=("arbitrary",), vmem_limit_bytes=63 * 2**20),
        cost_estimate=pl.CostEstimate(flops=9 * 2 * tokens * d * ff, bytes_accessed=100 * 2**20, transcendentals=0),
    )(x, dy, wg, wu, wd)
MESH = pl.DeviceIdType.MESH
CHUNKS = (("gate", 1), ("up", 1), ("down", 1), ("gate", 0), ("up", 0), ("down", 0))
FT = 512
SPLIT = (1, 1, 1, 1, 1, 2)
PERIOD, STEP, TILE = 14.0, 4.0, 1.7


def adamw(w, m, v, g):
    m = 0.9 * m + 0.1 * g
    v = 0.95 * v + 0.05 * g * g
    step = m * lax.rsqrt(v + 1e-8) + 0.1 * w
    return (w - 0.02 * step).astype(BF16), m, v


class Chunk:
    def __init__(self, place, bufs, own, ssem, rsem, free):
        self.__dict__.update(place)
        (self.T, self.D, self.YA, self.EA, self.FA, self.EB, self.FB, self.YB) = bufs
        self.w, self.m, self.v = own
        self.ssem, self.rsem, self.free = ssem, rsem, free
        self.R = self.T.shape[3]
        self.RA = self.R * 3 // 5
        self.A, self.B = pl.ds(0, self.RA), pl.ds(self.RA, self.R - self.RA)
        self.sent = []

    def copy(self, src, dst, s, r, dev):
        return pltpu.make_async_remote_copy(src_ref=src, dst_ref=dst, send_sem=self.ssem.at[s], recv_sem=self.rsem.at[r], device_id=dev, device_id_type=MESH)

    def send(self, cond, src, dst, s, r, dev):
        base, o = s if isinstance(s, tuple) else (s, None)
        self.copy(src, dst, base if o is None else base + o, r, dev).start()
        self.sent.append((cond, src.shape, base, o))

    def wait_sent(self):
        R, RA = self.R, self.RA
        like = {
            (2, 4, R): lambda: self.D,
            (RA,): lambda: self.YA.at[0],
            (R - RA,): lambda: self.YB,
            (2, R - RA): lambda: self.EB.at[0],
        }
        for cond, shape, base, o in self.sent[1:]:
            def wait():
                ref = like[tuple(shape[:-1])]()
                self.copy(ref, ref, base if o is None else base + o, 0, self.partner).wait_send()

            self.when(cond, wait)

    def got(self, dst, r):
        self.copy(dst, dst, 0, r, self.partner).wait_recv()

    def when(self, cond, f):
        if cond is None:
            f()
        else:
            pl.when(cond)(f)

    def add(self, dst, *srcs):
        dst[...] = sum(s[...].astype(F32) for s in (dst, *srcs)).astype(BF16)

    def own_y(self, o, rows):
        return self.T.at[self.y, o, self.c, rows, :]

    def both(self, o):
        return self.T.at[:, o, self.c, self.B, :]

    def s0(self):
        self.send(None, self.T.at[:, :, 1 - self.c], self.D, 0, 0, self.partner)

    def s1(self):
        self.got(self.D, 0)
        for n, o in enumerate((self.e1, self.i1, self.i0, self.e0)):
            t = self.D.at[1 - self.y, o, self.A, :]
            self.add(t, self.T.at[1 - self.y, o, self.c, self.A, :])
            self.send(None, t, self.YA.at[o], (1, o), 1 + o, self.across)

        def end():
            for slot, o in enumerate((self.e1, self.i1, self.i0)):
                t = self.D.at[:, o, self.B, :]
                self.add(t, self.both(o))
                self.send(self.end, t, self.EB.at[slot], 11 + slot, 11 + slot, self.inner)

        self.when(self.end, end)

    def s2(self):
        self.copy(self.D, self.D, 0, 0, self.partner).wait_send()
        pl.semaphore_signal(self.free, inc=1, device_id=self.partner, device_id_type=MESH)

        def mid():
            for slot, o in enumerate((self.e1, self.i1)):
                self.got(self.EB.at[slot], 11 + slot)
                t = self.D.at[:, o, self.B, :]
                self.add(t, self.both(o), self.EB.at[slot])
                self.send(self.mid, t, self.FB.at[slot], 14 + slot, 14 + slot, self.inner)

        self.when(self.mid, mid)

    def got_y(self, o):
        self.got(self.YA.at[o], 1 + o)

    def s3(self):
        def end():
            for slot, o in enumerate((self.e1, self.i1, self.i0)):
                self.got_y(o)
                t = self.YA.at[o]
                self.add(t, self.own_y(o, self.A), self.D.at[self.y, o, self.A, :])
                self.send(self.end, t, self.EA.at[slot], 5 + slot, 5 + slot, self.inner)

        def mid():
            self.got(self.FB.at[0], 14)
            t = self.D.at[:, self.e0, self.B, :]
            self.add(t, self.both(self.e0), self.FB.at[0])
            self.send(self.mid, t, self.FB.at[1], 16, 16, self.outer)

        self.when(self.end, end)
        self.when(self.mid, mid)

    def s4(self):
        def mid():
            for slot, o in enumerate((self.e1, self.i1)):
                self.got(self.EA.at[slot], 5 + slot)
                self.got_y(o)
                t = self.YA.at[o]
                self.add(t, self.own_y(o, self.A), self.D.at[self.y, o, self.A, :], self.EA.at[slot])
                self.send(self.mid, t, self.FA.at[slot], 8 + slot, 8 + slot, self.inner)

        self.when(self.mid, mid)
        own = self.T.at[1 - self.y, self.z, self.c, self.B, :]
        d = self.D.at[1 - self.y, self.z, self.B, :]
        t = self.FB.at[1, 1 - self.y]

        def mid2():
            self.got(self.FB.at[1], 15)
            self.got(self.EB.at[2], 13)
            self.add(t, own, d, self.EB.at[2, 1 - self.y])

        def end2():
            self.got(self.FB.at[1], 16)
            self.add(t, own, d)

        self.when(self.mid, mid2)
        self.when(self.end, end2)
        self.send(None, t, self.YB, 17, 17, self.across)

    def step(self, rows, *srcs):
        t = self.own_y(self.z, rows)
        g = sum(s[...].astype(F32) for s in (t, *srcs)).astype(BF16).astype(F32)
        w, m, v = adamw(self.w[rows, :].astype(F32), self.m[rows, :], self.v[rows, :], g)
        t[...] = w
        self.m[rows, :] = m
        self.v[rows, :] = v

    def s5(self):
        def mid():
            self.got(self.FA.at[0], 8)
            self.got_y(self.e0)
            t = self.YA.at[self.e0]
            self.add(t, self.own_y(self.e0, self.A), self.D.at[self.y, self.e0, self.A, :], self.FA.at[0])
            self.send(self.mid, t, self.FA.at[1], 10, 10, self.outer)

        self.when(self.mid, mid)
        self.got(self.YB, 17)
        d = self.D.at[self.y, self.z, self.B, :]
        self.when(self.mid, lambda: self.step(self.B, d, self.YB, self.FB.at[1, self.y], self.EB.at[2, self.y]))
        self.when(self.end, lambda: self.step(self.B, d, self.YB, self.FB.at[1, self.y]))
        t = self.own_y(self.z, self.B)
        self.send(None, t, t, 30, 30, self.across)

    def s6(self):
        self.got_y(self.z)
        d = self.D.at[self.y, self.z, self.A, :]

        def mid():
            self.got(self.FA.at[1], 9)
            self.got(self.EA.at[2], 7)
            self.step(self.A, d, self.YA.at[self.z], self.FA.at[1], self.EA.at[2])

        def end():
            self.got(self.FA.at[1], 10)
            self.step(self.A, d, self.YA.at[self.z], self.FA.at[1])

        self.when(self.mid, mid)
        self.when(self.end, end)
        self.give_a(self.z, None, self.mid, None)
        self.got(self.T.at[1 - self.y, self.z, self.c, self.B, :], 30)
        self.give_b(self.z, None, self.mid)

    def give_a(self, o, inward, outward, cond):
        t = self.own_y(o, self.A)
        if inward is not False:
            self.when(inward, lambda: self.send(inward, t, t, (18, o), 18 + o, self.inner))
        if outward is not False:
            self.when(outward, lambda: self.send(outward, t, t, (22, o), 18 + o, self.outer))
        self.send(cond, t, t, (26, o), 26 + o, self.across)

    def give_b(self, o, inward, outward):
        t = self.both(o)
        if inward is not False:
            self.when(inward, lambda: self.send(inward, t, t, (31, o), 31 + o, self.inner))
        if outward is not False:
            self.when(outward, lambda: self.send(outward, t, t, (35, o), 31 + o, self.outer))

    def got_a(self, o):
        self.got(self.own_y(o, self.A), 18 + o)

    def got_b(self, o):
        self.got(self.both(o), 31 + o)

    def plain(self, cond, o, inward, outward, which):
        if which == "a":
            t = self.own_y(o, self.A)
            self.got_a(o)
            base = 18
        else:
            t = self.both(o)
            self.got_b(o)
            base = 31
        if inward:
            self.send(cond, t, t, (base, o), base + o, self.inner)
        if outward:
            self.send(cond, t, t, (base + 4, o), base + o, self.outer)
        if which == "a":
            self.send(cond, t, t, (26, o), 26 + o, self.across)

    def g1(self, which):
        def mid():
            self.plain(self.mid, self.e0, True, False, which)
            self.plain(self.mid, self.i1, False, True, which)

        self.when(self.mid, mid)
        self.when(self.end, lambda: self.plain(self.end, self.i0, False, False, which))

    def g2(self, which):
        self.when(self.mid, lambda: self.plain(self.mid, self.e1, False, True, which))
        self.when(self.end, lambda: self.plain(self.end, self.i1, False, False, which))

    def g3(self, which):
        self.when(self.end, lambda: self.plain(self.end, self.e1, False, False, which))

    def s7(self):
        self.g1("a")

    def s8(self):
        self.g1("b")
        self.g2("a")

    def s9(self):
        self.g2("b")
        self.g3("a")

    def s10(self):
        self.g3("b")
        for o in range(4):
            self.got(self.T.at[1 - self.y, o, self.c, self.A, :], 26 + o)
        pl.semaphore_wait(self.free, 1)
        t = self.T.at[:, :, self.c]
        self.send(None, t, t, 39, 39, self.partner)

    def s11(self):
        self.got(self.T.at[:, :, 1 - self.c], 39)
        self.wait_sent()

    STEPS = ("s0", "s1", "s2", "s3", "s4", "s5", "s6", "s7", "s8", "s9", "s10", "s11")


def kernel(act2, dg2, du2, act1, dg1, du1, at1, at2, dyt, dht, wg, wu, wd, mg, mu, md, vg, vu, vd,
           tg, tu, td, sm_g, sm_u, sm_d, sv_g, sv_u, sv_d,
           dG, dDn, yaG, yaD, eaG, eaD, faG, faD, ebG, ebD, fbG, fbD, ybG, ybD,
           lhs, rhs, sw_g, sw_u, sw_d,
           ssem, rsem, lsem, tsem, isem, free):
    rep, me = lax.axis_index("rep"), lax.axis_index("dp")
    c, z, y = me % 2, (me // 2) % 4, me // 8

    def dev(y, z, c):
        return (rep, y * 8 + z * 2 + c)

    low = z < 2
    e0, i0, i1, e1 = (jnp.where(low, p, 3 - p) for p in range(4))
    end = (z == 0) | (z == 3)
    mid = (z == 1) | (z == 2)
    inner = dev(y, jnp.where(end, i0, i1), c)
    outer = dev(y, e0, c)
    place = dict(y=y, z=z, c=c, e0=e0, i0=i0, i1=i1, e1=e1, end=end, mid=mid, inner=inner, outer=outer, across=dev(1 - y, z, c), partner=dev(y, z, 1 - c))

    owns = {"gate": (sw_g, sm_g, sv_g), "up": (sw_u, sm_u, sv_u), "down": (sw_d, sm_d, sv_d)}
    T = {"gate": tg, "up": tu, "down": td}
    loads = []
    for n, (name, hw, hm, hv) in enumerate((("gate", wg, mg, vg), ("up", wu, mu, vu), ("down", wd, md, vd))):
        sw, sm, sv = owns[name]
        loads += [pltpu.make_async_copy(hw.at[:, me], sw, isem.at[n, 0]), pltpu.make_async_copy(hm, sm, isem.at[n, 1]), pltpu.make_async_copy(hv, sv, isem.at[n, 2])]

    left = {("down", 1): dyt, ("gate", 1): at2, ("up", 1): at2, ("down", 0): dht, ("gate", 0): at1, ("up", 0): at1}
    right = {("down", 1): act2, ("gate", 1): dg2, ("up", 1): du2, ("down", 0): act1, ("gate", 0): dg1, ("up", 0): du1}
    tiles = right[CHUNKS[0]].shape[1] // FT

    def rhs_copy(k, j):
        t = tiles * k + j
        return pltpu.make_async_copy(right[CHUNKS[k]].at[:, pl.ds(j * FT, FT)], rhs.at[t % 2], tsem.at[t % 2])

    def lhs_copy(k):
        s = 0 if CHUNKS[k][0] == "down" else 1
        return pltpu.make_async_copy(left[CHUNKS[k]], lhs.at[s], lsem.at[s])

    lhs_copy(0).start()
    rhs_copy(0, 0).start()
    lhs_copy(2).start()

    barrier = pltpu.get_barrier_semaphore()
    for d, cond in ((place["partner"], None), (place["across"], None), (inner, None), (outer, mid)):
        if cond is None:
            pl.semaphore_signal(barrier, inc=1, device_id=d, device_id_type=MESH)
        else:
            @pl.when(cond)
            def _():
                pl.semaphore_signal(barrier, inc=1, device_id=d, device_id_type=MESH)
    pl.when(mid)(lambda: pl.semaphore_wait(barrier, 4))
    pl.when(end)(lambda: pl.semaphore_wait(barrier, 3))

    def part(k, ref, h):
        if SPLIT[k] == 1:
            return ref
        rows, cols = ref.shape[-2] // SPLIT[k], ref.shape[-1] // SPLIT[k]
        lead = (slice(None),) * (len(ref.shape) - 2)
        if CHUNKS[k][0] == "down":
            return ref.at[lead + (pl.ds(h * rows, rows), slice(None))]
        return ref.at[lead + (slice(None), pl.ds(h * cols, cols))]

    chunks, which = [], []
    counts = [0, 0]
    for k, (name, l) in enumerate(CHUNKS):
        pick = 1 if name == "down" else 0
        n = counts[pick]
        counts[pick] += 1
        for h in range(SPLIT[k]):
            bufs = [T[name].at[l]] + [b[pick].at[n] for b in ((dG, dDn), (yaG, yaD), (eaG, eaD), (faG, faD), (ebG, ebD), (fbG, fbD), (ybG, ybD))]
            i = len(chunks)
            chunks.append(Chunk(place, [part(k, b, h) for b in bufs], [part(k, b.at[l], h) for b in owns[name]], ssem.at[i], rsem.at[i], free.at[i]))
            which.append((k, h))

    def run(k, s):
        if (k, s) == (0, 5):
            for cp in loads:
                cp.wait()
        getattr(chunks[k], Chunk.STEPS[s])()

    def ready(i):
        k, h = which[i]
        return tiles * (k + 1) - 1 if CHUNKS[k][0] == "down" else tiles * k - (-tiles * (h + 1) // SPLIT[k]) - 1

    plan = sorted((max(ready(i), ready(0) + (PERIOD * (which[i][0] + which[i][1] / SPLIT[which[i][0]]) + STEP * s) / TILE) + s * 1e-6, i, s) for i in range(len(chunks)) for s in range(len(Chunk.STEPS)))
    total_tiles = tiles * len(CHUNKS)
    slots = {}
    for at, k, s in plan:
        slots.setdefault(min(int(at), total_tiles), []).append((k, s))

    for k, (name, l) in enumerate(CHUNKS):
        if k == 0:
            for cp in loads:
                cp.start()
        if k in (0, 2, 3, 5):
            lhs_copy(k).wait()
        side = 0 if name == "down" else 1

        def tile(j, _, k=k, name=name, l=l, side=side):
            t = tiles * k + j
            rhs_copy(k, j).wait()

            @pl.when(j < tiles - 1)
            def _():
                rhs_copy(k, j + 1).start()

            if k + 1 < len(CHUNKS):
                @pl.when(j == tiles - 1)
                def _():
                    rhs_copy(k + 1, 0).start()

            out = jnp.dot(lhs[side], rhs[t % 2], preferred_element_type=F32).astype(BF16)
            if name == "down":
                out = out.T
                for q in range(FT // 32):
                    n = (FT // 32) * j + q
                    b, r = n // 5, pl.multiple_of((n % 5) * 32, 32)
                    td[l, b // 8, (b // 2) % 4, b % 2, pl.ds(r, 32), :] = out[32 * q : 32 * q + 32]
            else:
                T[name][l, :, :, :, :, pl.ds(pl.multiple_of(j * FT, FT), FT)] = out.reshape(2, 4, 2, 40, FT)
            for jj in range(tiles):
                todo = slots.get(tiles * k + jj, [])
                if todo:
                    @pl.when(j == jj)
                    def _(todo=todo):
                        for kk, s in todo:
                            run(kk, s)
            return 0

        lax.fori_loop(0, tiles, tile, 0)
        if k in (1, 2):
            lhs_copy(2 * k + 1).start()
    for kk, s in slots.get(total_tiles, []):
        run(kk, s)


def comm(parts, weights, moments, ):
    hbm = pl.BlockSpec(memory_space=pl.ANY)
    wg, wu, wd = weights
    blocks = [w.reshape(w.shape[0], 16, w.shape[1] // 16, w.shape[2]) for w in weights]
    outs = [pltpu.VMEM((2, 2, 4, 2) + b.shape[2:], BF16) for b in blocks]
    outs += [pltpu.VMEM(t.shape, F32) for t in moments]
    g, d = (40, 2560), (160, 640)

    def pair(*lead, a=None):
        def rows(s):
            return {None: s[0], "A": s[0] * 3 // 5, "B": s[0] * 2 // 5}[a]
        return [pltpu.VMEM((4, *lead, rows(g), g[1]), BF16), pltpu.VMEM((2, *lead, rows(d), d[1]), BF16)]

    scratch = pair(2, 4) + pair(4, a="A") + pair(3, a="A") + pair(2, a="A") + pair(3, 2, a="B") + pair(2, 2, a="B") + pair(a="B")
    scratch += [pltpu.VMEM((2, 640, 2048), BF16), pltpu.VMEM((2, 2048, FT), BF16)]
    scratch += [pltpu.VMEM((2,) + b.shape[2:], BF16) for b in blocks]
    dma = pltpu.SemaphoreType.DMA
    scratch += [dma((sum(SPLIT), 40)), dma((sum(SPLIT), 40)), dma((2,)), dma((2,)), dma((3, 3)), pltpu.SemaphoreType.REGULAR((sum(SPLIT),))]
    return pl.pallas_call(
        kernel,
        in_specs=[hbm] * 19,
        out_specs=[pl.BlockSpec(memory_space=pltpu.VMEM)] * 9,
        out_shape=outs,
        scratch_shapes=scratch,
        compiler_params=pltpu.CompilerParams(collective_id=0, has_side_effects=True, vmem_limit_bytes=38 * 2**20),
        cost_estimate=pl.CostEstimate(flops=6 * 2 * 2048 * 640 * 2560, bytes_accessed=100 * 2**20, transcendentals=0),
    )(*parts, *blocks, *moments)


def put_kernel(*refs):
    n = len(refs) // 2
    copies = [pltpu.make_async_copy(src, dst, refs[-1].at[i]) for i, (src, dst) in enumerate(zip(refs[:n], refs[n : 2 * n]))]
    for c in copies:
        c.start()
    for c in copies:
        c.wait()


def put(arrays):
    return pl.pallas_call(
        put_kernel,
        in_specs=[pl.BlockSpec(memory_space=pltpu.VMEM)] * len(arrays),
        out_specs=[pl.BlockSpec(memory_space=pltpu.HBM)] * len(arrays),
        out_shape=[jax.ShapeDtypeStruct(a.shape, a.dtype) for a in arrays],
        scratch_shapes=[pltpu.SemaphoreType.DMA((len(arrays),))],
        compiler_params=pltpu.CompilerParams(vmem_limit_bytes=2**20),
    )(*arrays)


def solution(mesh):
    def step(x, dy, wg, wu, wd, *moments):
        parts = chain(x[0], dy[0], wg, wu, wd)
        new = put(comm(parts, (wg, wu, wd), moments))
        return tuple(t.reshape(w.shape) for t, w in zip(new, (wg, wu, wd))) + tuple(new[3:])

    whole, rows = P(None, None, None), P(None, "dp", None)
    return jax.shard_map(
        step,
        mesh=mesh,
        in_specs=(P(("rep", "dp")),) * 2 + (whole,) * 3 + (rows,) * 6,
        out_specs=(P("rep", None, None),) * 3 + (P("rep", "dp", None),) * 6,
        check_vma=False,
    )
```

```python
import jax
import jax.numpy as jnp
from jax import lax
from jax.experimental import pallas as pl
from jax.experimental.pallas import tpu as pltpu
from jax.sharding import PartitionSpec as P

F32, BF16 = jnp.float32, jnp.bfloat16
NT = (((1,), (1,)), ((), ()))


def dot(a, b):
    return jnp.dot(a, b, preferred_element_type=F32)


def dot_t(a, b):
    return lax.dot_general(a, b, NT, preferred_element_type=F32)


def sigmoid(x):
    return 0.5 * jnp.tanh(0.5 * x) + 0.5


def norm_scale(h):
    wide = h.astype(F32)
    return wide, lax.rsqrt(jnp.mean(wide * wide, -1, keepdims=True) + 1e-6)


def chain_kernel(x_ref, dy_ref, wg_hbm, wu_hbm, wd_hbm, act2_ref, dg2_ref, du2_ref, act1_ref, dg1_ref, du1_ref, at1_ref, at2_ref, dyt_ref, dht_ref,
                 wg, wu, wd, gate1, up1, sems, *, ft):
    ff = wg.shape[2]
    i = pl.program_id(0)
    copies = [pltpu.make_async_copy(src.at[l], dst.at[l], sems.at[l, k]) for l in range(2) for k, (src, dst) in enumerate(((wg_hbm, wg), (wu_hbm, wu), (wd_hbm, wd)))]

    @pl.when(i == 0)
    def _():
        for c in copies:
            c.start()

    def arrived(n):
        @pl.when(i == 0)
        def _():
            copies[n].wait()

    x = x_ref[...]
    dy = dy_ref[...]
    wide, s = norm_scale(x)
    a = (wide * s).astype(BF16)
    at1_ref[...] = a.T
    dyt_ref[...] = dy.T
    arrived(0)
    arrived(1)
    total = jnp.zeros(x.shape, F32)
    for f in range(0, ff, ft):
        fs = pl.ds(f, ft)
        gate = dot(a, wg[0, :, fs])
        up = dot(a, wu[0, :, fs])
        gate1[:, fs] = gate
        up1[:, fs] = up
        act = (gate * sigmoid(gate) * up).astype(BF16)
        act1_ref[:, fs] = act
        if f == 0:
            arrived(2)
        total += dot(act, wd[0, fs, :])
    h = x + total.astype(BF16)
    arrived(3)
    arrived(4)
    arrived(5)
    wide, s = norm_scale(h)
    a = (wide * s).astype(BF16)
    at2_ref[...] = a.T
    dag = jnp.zeros(x.shape, F32)
    dau = jnp.zeros(x.shape, F32)

    def back(dout, gate, up, l, fs, refs):
        dact = dot_t(dout, wd[l, fs, :]).astype(BF16).astype(F32)
        sig = sigmoid(gate)
        silu = gate * sig
        du = (dact * silu).astype(BF16)
        dg = (dact * up * (sig + silu * (1.0 - sig))).astype(BF16)
        refs[0][:, fs] = dg
        refs[1][:, fs] = du
        return dg, du, silu

    for f in range(0, ff, ft):
        fs = pl.ds(f, ft)
        gate = dot(a, wg[1, :, fs])
        up = dot(a, wu[1, :, fs])
        dg, du, silu = back(dy, gate, up, 1, fs, (dg2_ref, du2_ref))
        act2_ref[:, fs] = (silu * up).astype(BF16)
        dag += dot_t(dg, wg[1, :, fs])
        dau += dot_t(du, wu[1, :, fs])
    da = (dag.astype(BF16) + dau.astype(BF16)).astype(F32)
    inner = jnp.mean(da * wide, -1, keepdims=True)
    dh = dy + (da * s - wide * (s * s * s * inner)).astype(BF16)
    dht_ref[...] = dh.T
    for f in range(0, ff, ft):
        fs = pl.ds(f, ft)
        back(dh, gate1[:, fs], up1[:, fs], 0, fs, (dg1_ref, du1_ref))


def chain(x, dy, wg, wu, wd, tile=256, ft=1280):
    tokens, d = x.shape
    ff = wg.shape[2]
    rows = pl.BlockSpec((tile, d), lambda i: (i, 0))
    cols = pl.BlockSpec((d, tile), lambda i: (0, i))
    wide = pl.BlockSpec((tile, ff), lambda i: (i, 0))
    hbm = pl.BlockSpec(memory_space=pl.ANY)
    return pl.pallas_call(
        lambda *r: chain_kernel(*r, ft=ft),
        grid=(tokens // tile,),
        in_specs=[rows, rows, hbm, hbm, hbm],
        out_specs=[wide] * 6 + [cols] * 4,
        out_shape=[jax.ShapeDtypeStruct((tokens, ff), BF16)] * 6 + [jax.ShapeDtypeStruct((d, tokens), BF16)] * 4,
        scratch_shapes=[pltpu.VMEM(wg.shape, BF16), pltpu.VMEM(wu.shape, BF16), pltpu.VMEM(wd.shape, BF16), pltpu.VMEM((tile, ff), F32), pltpu.VMEM((tile, ff), F32), pltpu.SemaphoreType.DMA((2, 3))],
        compiler_params=pltpu.CompilerParams(dimension_semantics=("arbitrary",), vmem_limit_bytes=63 * 2**20),
        cost_estimate=pl.CostEstimate(flops=9 * 2 * tokens * d * ff, bytes_accessed=100 * 2**20, transcendentals=0),
    )(x, dy, wg, wu, wd)
MESH = pl.DeviceIdType.MESH
CHUNKS = (("gate", 1), ("up", 1), ("down", 1), ("gate", 0), ("up", 0), ("down", 0))
FT = 512
SPLIT = (2, 1, 1, 1, 1, 2)
PERIOD, STEP, TILE = 13.0, 4.0, 1.7


def adamw(w, m, v, g):
    m = 0.9 * m + 0.1 * g
    v = 0.95 * v + 0.05 * g * g
    step = m * lax.rsqrt(v + 1e-8) + 0.1 * w
    return (w - 0.02 * step).astype(BF16), m, v


class Chunk:
    def __init__(self, place, bufs, own, ssem, rsem, free):
        self.__dict__.update(place)
        (self.T, self.D, self.YA, self.EA, self.FA, self.EB, self.FB, self.YB) = bufs
        self.w, self.m, self.v = own
        self.ssem, self.rsem, self.free = ssem, rsem, free
        self.R = self.T.shape[3]
        self.RA = self.R * 3 // 5
        self.A, self.B = pl.ds(0, self.RA), pl.ds(self.RA, self.R - self.RA)
        self.sent = []

    def copy(self, src, dst, s, r, dev):
        return pltpu.make_async_remote_copy(src_ref=src, dst_ref=dst, send_sem=self.ssem.at[s], recv_sem=self.rsem.at[r], device_id=dev, device_id_type=MESH)

    def send(self, cond, src, dst, s, r, dev):
        base, o = s if isinstance(s, tuple) else (s, None)
        self.copy(src, dst, base if o is None else base + o, r, dev).start()
        self.sent.append((cond, src.shape, base, o))

    def wait_sent(self):
        R, RA = self.R, self.RA
        like = {
            (2, 4, R): lambda: self.D,
            (RA,): lambda: self.YA.at[0],
            (R - RA,): lambda: self.YB,
            (2, R - RA): lambda: self.EB.at[0],
        }
        for cond, shape, base, o in self.sent[1:]:
            def wait():
                ref = like[tuple(shape[:-1])]()
                self.copy(ref, ref, base if o is None else base + o, 0, self.partner).wait_send()

            self.when(cond, wait)

    def got(self, dst, r):
        self.copy(dst, dst, 0, r, self.partner).wait_recv()

    def when(self, cond, f):
        if cond is None:
            f()
        else:
            pl.when(cond)(f)

    def add(self, dst, *srcs):
        dst[...] = sum(s[...].astype(F32) for s in (dst, *srcs)).astype(BF16)

    def own_y(self, o, rows):
        return self.T.at[self.y, o, self.c, rows, :]

    def both(self, o):
        return self.T.at[:, o, self.c, self.B, :]

    def s0(self):
        self.send(None, self.T.at[:, :, 1 - self.c], self.D, 0, 0, self.partner)

    def s1(self):
        self.got(self.D, 0)
        for n, o in enumerate((self.e1, self.i1, self.i0, self.e0)):
            t = self.D.at[1 - self.y, o, self.A, :]
            self.add(t, self.T.at[1 - self.y, o, self.c, self.A, :])
            self.send(None, t, self.YA.at[o], (1, o), 1 + o, self.across)

        def end():
            for slot, o in enumerate((self.e1, self.i1, self.i0)):
                t = self.D.at[:, o, self.B, :]
                self.add(t, self.both(o))
                self.send(self.end, t, self.EB.at[slot], 11 + slot, 11 + slot, self.inner)

        self.when(self.end, end)

    def s2(self):
        self.copy(self.D, self.D, 0, 0, self.partner).wait_send()
        pl.semaphore_signal(self.free, inc=1, device_id=self.partner, device_id_type=MESH)

        def mid():
            for slot, o in enumerate((self.e1, self.i1)):
                self.got(self.EB.at[slot], 11 + slot)
                t = self.D.at[:, o, self.B, :]
                self.add(t, self.both(o), self.EB.at[slot])
                self.send(self.mid, t, self.FB.at[slot], 14 + slot, 14 + slot, self.inner)

        self.when(self.mid, mid)

    def got_y(self, o):
        self.got(self.YA.at[o], 1 + o)

    def s3(self):
        def end():
            for slot, o in enumerate((self.e1, self.i1, self.i0)):
                self.got_y(o)
                t = self.YA.at[o]
                self.add(t, self.own_y(o, self.A), self.D.at[self.y, o, self.A, :])
                self.send(self.end, t, self.EA.at[slot], 5 + slot, 5 + slot, self.inner)

        def mid():
            self.got(self.FB.at[0], 14)
            t = self.D.at[:, self.e0, self.B, :]
            self.add(t, self.both(self.e0), self.FB.at[0])
            self.send(self.mid, t, self.FB.at[1], 16, 16, self.outer)

        self.when(self.end, end)
        self.when(self.mid, mid)

    def s4(self):
        def mid():
            for slot, o in enumerate((self.e1, self.i1)):
                self.got(self.EA.at[slot], 5 + slot)
                self.got_y(o)
                t = self.YA.at[o]
                self.add(t, self.own_y(o, self.A), self.D.at[self.y, o, self.A, :], self.EA.at[slot])
                self.send(self.mid, t, self.FA.at[slot], 8 + slot, 8 + slot, self.inner)

        self.when(self.mid, mid)
        own = self.T.at[1 - self.y, self.z, self.c, self.B, :]
        d = self.D.at[1 - self.y, self.z, self.B, :]
        t = self.FB.at[1, 1 - self.y]

        def mid2():
            self.got(self.FB.at[1], 15)
            self.got(self.EB.at[2], 13)
            self.add(t, own, d, self.EB.at[2, 1 - self.y])

        def end2():
            self.got(self.FB.at[1], 16)
            self.add(t, own, d)

        self.when(self.mid, mid2)
        self.when(self.end, end2)
        self.send(None, t, self.YB, 17, 17, self.across)

    def step(self, rows, *srcs):
        t = self.own_y(self.z, rows)
        g = sum(s[...].astype(F32) for s in (t, *srcs)).astype(BF16).astype(F32)
        w, m, v = adamw(self.w[rows, :].astype(F32), self.m[rows, :], self.v[rows, :], g)
        t[...] = w
        self.m[rows, :] = m
        self.v[rows, :] = v

    def s5(self):
        def mid():
            self.got(self.FA.at[0], 8)
            self.got_y(self.e0)
            t = self.YA.at[self.e0]
            self.add(t, self.own_y(self.e0, self.A), self.D.at[self.y, self.e0, self.A, :], self.FA.at[0])
            self.send(self.mid, t, self.FA.at[1], 10, 10, self.outer)

        self.when(self.mid, mid)
        self.got(self.YB, 17)
        d = self.D.at[self.y, self.z, self.B, :]
        self.when(self.mid, lambda: self.step(self.B, d, self.YB, self.FB.at[1, self.y], self.EB.at[2, self.y]))
        self.when(self.end, lambda: self.step(self.B, d, self.YB, self.FB.at[1, self.y]))
        t = self.own_y(self.z, self.B)
        self.send(None, t, t, 30, 30, self.across)

    def s6(self):
        self.got_y(self.z)
        d = self.D.at[self.y, self.z, self.A, :]

        def mid():
            self.got(self.FA.at[1], 9)
            self.got(self.EA.at[2], 7)
            self.step(self.A, d, self.YA.at[self.z], self.FA.at[1], self.EA.at[2])

        def end():
            self.got(self.FA.at[1], 10)
            self.step(self.A, d, self.YA.at[self.z], self.FA.at[1])

        self.when(self.mid, mid)
        self.when(self.end, end)
        self.give_a(self.z, None, self.mid, None)
        self.got(self.T.at[1 - self.y, self.z, self.c, self.B, :], 30)
        self.give_b(self.z, None, self.mid)

    def give_a(self, o, inward, outward, cond):
        t = self.own_y(o, self.A)
        if inward is not False:
            self.when(inward, lambda: self.send(inward, t, t, (18, o), 18 + o, self.inner))
        if outward is not False:
            self.when(outward, lambda: self.send(outward, t, t, (22, o), 18 + o, self.outer))
        self.send(cond, t, t, (26, o), 26 + o, self.across)

    def give_b(self, o, inward, outward):
        t = self.both(o)
        if inward is not False:
            self.when(inward, lambda: self.send(inward, t, t, (31, o), 31 + o, self.inner))
        if outward is not False:
            self.when(outward, lambda: self.send(outward, t, t, (35, o), 31 + o, self.outer))

    def got_a(self, o):
        self.got(self.own_y(o, self.A), 18 + o)

    def got_b(self, o):
        self.got(self.both(o), 31 + o)

    def plain(self, cond, o, inward, outward, which):
        if which == "a":
            t = self.own_y(o, self.A)
            self.got_a(o)
            base = 18
        else:
            t = self.both(o)
            self.got_b(o)
            base = 31
        if inward:
            self.send(cond, t, t, (base, o), base + o, self.inner)
        if outward:
            self.send(cond, t, t, (base + 4, o), base + o, self.outer)
        if which == "a":
            self.send(cond, t, t, (26, o), 26 + o, self.across)

    def g1(self, which):
        def mid():
            self.plain(self.mid, self.e0, True, False, which)
            self.plain(self.mid, self.i1, False, True, which)

        self.when(self.mid, mid)
        self.when(self.end, lambda: self.plain(self.end, self.i0, False, False, which))

    def g2(self, which):
        self.when(self.mid, lambda: self.plain(self.mid, self.e1, False, True, which))
        self.when(self.end, lambda: self.plain(self.end, self.i1, False, False, which))

    def g3(self, which):
        self.when(self.end, lambda: self.plain(self.end, self.e1, False, False, which))

    def s7(self):
        self.g1("a")

    def s8(self):
        self.g1("b")
        self.g2("a")

    def s9(self):
        self.g2("b")
        self.g3("a")

    def s10(self):
        self.g3("b")
        for o in range(4):
            self.got(self.T.at[1 - self.y, o, self.c, self.A, :], 26 + o)
        pl.semaphore_wait(self.free, 1)
        t = self.T.at[:, :, self.c]
        self.send(None, t, t, 39, 39, self.partner)

    def s11(self):
        self.got(self.T.at[:, :, 1 - self.c], 39)
        self.wait_sent()

    STEPS = ("s0", "s1", "s2", "s3", "s4", "s5", "s6", "s7", "s8", "s9", "s10", "s11")


def kernel(act2, dg2, du2, act1, dg1, du1, at1, at2, dyt, dht, wg, wu, wd, mg, mu, md, vg, vu, vd,
           tg, tu, td, sm_g, sm_u, sm_d, sv_g, sv_u, sv_d,
           dG, dDn, yaG, yaD, eaG, eaD, faG, faD, ebG, ebD, fbG, fbD, ybG, ybD,
           lhs, rhs, sw_g, sw_u, sw_d,
           ssem, rsem, lsem, tsem, isem, free):
    rep, me = lax.axis_index("rep"), lax.axis_index("dp")
    c, z, y = me % 2, (me // 2) % 4, me // 8

    def dev(y, z, c):
        return (rep, y * 8 + z * 2 + c)

    low = z < 2
    e0, i0, i1, e1 = (jnp.where(low, p, 3 - p) for p in range(4))
    end = (z == 0) | (z == 3)
    mid = (z == 1) | (z == 2)
    inner = dev(y, jnp.where(end, i0, i1), c)
    outer = dev(y, e0, c)
    place = dict(y=y, z=z, c=c, e0=e0, i0=i0, i1=i1, e1=e1, end=end, mid=mid, inner=inner, outer=outer, across=dev(1 - y, z, c), partner=dev(y, z, 1 - c))

    owns = {"gate": (sw_g, sm_g, sv_g), "up": (sw_u, sm_u, sv_u), "down": (sw_d, sm_d, sv_d)}
    T = {"gate": tg, "up": tu, "down": td}
    loads = []
    for n, (name, hw, hm, hv) in enumerate((("gate", wg, mg, vg), ("up", wu, mu, vu), ("down", wd, md, vd))):
        sw, sm, sv = owns[name]
        loads += [pltpu.make_async_copy(hw.at[:, me], sw, isem.at[n, 0]), pltpu.make_async_copy(hm, sm, isem.at[n, 1]), pltpu.make_async_copy(hv, sv, isem.at[n, 2])]

    left = {("down", 1): dyt, ("gate", 1): at2, ("up", 1): at2, ("down", 0): dht, ("gate", 0): at1, ("up", 0): at1}
    right = {("down", 1): act2, ("gate", 1): dg2, ("up", 1): du2, ("down", 0): act1, ("gate", 0): dg1, ("up", 0): du1}
    tiles = right[CHUNKS[0]].shape[1] // FT

    def rhs_copy(k, j):
        t = tiles * k + j
        return pltpu.make_async_copy(right[CHUNKS[k]].at[:, pl.ds(j * FT, FT)], rhs.at[t % 2], tsem.at[t % 2])

    def lhs_copy(k):
        s = 0 if CHUNKS[k][0] == "down" else 1
        return pltpu.make_async_copy(left[CHUNKS[k]], lhs.at[s], lsem.at[s])

    lhs_copy(0).start()
    rhs_copy(0, 0).start()
    lhs_copy(2).start()

    barrier = pltpu.get_barrier_semaphore()
    for d, cond in ((place["partner"], None), (place["across"], None), (inner, None), (outer, mid)):
        if cond is None:
            pl.semaphore_signal(barrier, inc=1, device_id=d, device_id_type=MESH)
        else:
            @pl.when(cond)
            def _():
                pl.semaphore_signal(barrier, inc=1, device_id=d, device_id_type=MESH)
    pl.when(mid)(lambda: pl.semaphore_wait(barrier, 4))
    pl.when(end)(lambda: pl.semaphore_wait(barrier, 3))

    def part(k, ref, h):
        if SPLIT[k] == 1:
            return ref
        rows, cols = ref.shape[-2] // SPLIT[k], ref.shape[-1] // SPLIT[k]
        lead = (slice(None),) * (len(ref.shape) - 2)
        if CHUNKS[k][0] == "down":
            return ref.at[lead + (pl.ds(h * rows, rows), slice(None))]
        return ref.at[lead + (slice(None), pl.ds(h * cols, cols))]

    chunks, which = [], []
    counts = [0, 0]
    for k, (name, l) in enumerate(CHUNKS):
        pick = 1 if name == "down" else 0
        n = counts[pick]
        counts[pick] += 1
        for h in range(SPLIT[k]):
            bufs = [T[name].at[l]] + [b[pick].at[n] for b in ((dG, dDn), (yaG, yaD), (eaG, eaD), (faG, faD), (ebG, ebD), (fbG, fbD), (ybG, ybD))]
            i = len(chunks)
            chunks.append(Chunk(place, [part(k, b, h) for b in bufs], [part(k, b.at[l], h) for b in owns[name]], ssem.at[i], rsem.at[i], free.at[i]))
            which.append((k, h))

    def run(k, s):
        if (k, s) == (0, 5):
            for cp in loads:
                cp.wait()
        getattr(chunks[k], Chunk.STEPS[s])()

    def ready(i):
        k, h = which[i]
        return tiles * (k + 1) - 1 if CHUNKS[k][0] == "down" else tiles * k - (-tiles * (h + 1) // SPLIT[k]) - 1

    plan = sorted((max(ready(i), ready(0) + (PERIOD * (which[i][0] + which[i][1] / SPLIT[which[i][0]]) + STEP * s) / TILE) + s * 1e-6, i, s) for i in range(len(chunks)) for s in range(len(Chunk.STEPS)))
    total_tiles = tiles * len(CHUNKS)
    slots = {}
    for at, k, s in plan:
        slots.setdefault(min(int(at), total_tiles), []).append((k, s))

    for k, (name, l) in enumerate(CHUNKS):
        if k == 0:
            for cp in loads:
                cp.start()
        if k in (0, 2, 3, 5):
            lhs_copy(k).wait()
        side = 0 if name == "down" else 1

        def tile(j, _, k=k, name=name, l=l, side=side):
            t = tiles * k + j
            rhs_copy(k, j).wait()

            @pl.when(j < tiles - 1)
            def _():
                rhs_copy(k, j + 1).start()

            if k + 1 < len(CHUNKS):
                @pl.when(j == tiles - 1)
                def _():
                    rhs_copy(k + 1, 0).start()

            out = jnp.dot(lhs[side], rhs[t % 2], preferred_element_type=F32).astype(BF16)
            if name == "down":
                out = out.T
                for q in range(FT // 32):
                    n = (FT // 32) * j + q
                    b, r = n // 5, pl.multiple_of((n % 5) * 32, 32)
                    td[l, b // 8, (b // 2) % 4, b % 2, pl.ds(r, 32), :] = out[32 * q : 32 * q + 32]
            else:
                T[name][l, :, :, :, :, pl.ds(pl.multiple_of(j * FT, FT), FT)] = out.reshape(2, 4, 2, 40, FT)
            for jj in range(tiles):
                todo = slots.get(tiles * k + jj, [])
                if todo:
                    @pl.when(j == jj)
                    def _(todo=todo):
                        for kk, s in todo:
                            run(kk, s)
            return 0

        lax.fori_loop(0, tiles, tile, 0)
        if k in (1, 2):
            lhs_copy(2 * k + 1).start()
    for kk, s in slots.get(total_tiles, []):
        run(kk, s)


def comm(parts, weights, moments, ):
    hbm = pl.BlockSpec(memory_space=pl.ANY)
    wg, wu, wd = weights
    blocks = [w.reshape(w.shape[0], 16, w.shape[1] // 16, w.shape[2]) for w in weights]
    outs = [pltpu.VMEM((2, 2, 4, 2) + b.shape[2:], BF16) for b in blocks]
    outs += [pltpu.VMEM(t.shape, F32) for t in moments]
    g, d = (40, 2560), (160, 640)

    def pair(*lead, a=None):
        def rows(s):
            return {None: s[0], "A": s[0] * 3 // 5, "B": s[0] * 2 // 5}[a]
        return [pltpu.VMEM((4, *lead, rows(g), g[1]), BF16), pltpu.VMEM((2, *lead, rows(d), d[1]), BF16)]

    scratch = pair(2, 4) + pair(4, a="A") + pair(3, a="A") + pair(2, a="A") + pair(3, 2, a="B") + pair(2, 2, a="B") + pair(a="B")
    scratch += [pltpu.VMEM((2, 640, 2048), BF16), pltpu.VMEM((2, 2048, FT), BF16)]
    scratch += [pltpu.VMEM((2,) + b.shape[2:], BF16) for b in blocks]
    dma = pltpu.SemaphoreType.DMA
    scratch += [dma((sum(SPLIT), 40)), dma((sum(SPLIT), 40)), dma((2,)), dma((2,)), dma((3, 3)), pltpu.SemaphoreType.REGULAR((sum(SPLIT),))]
    return pl.pallas_call(
        kernel,
        in_specs=[hbm] * 19,
        out_specs=[pl.BlockSpec(memory_space=pltpu.VMEM)] * 9,
        out_shape=outs,
        scratch_shapes=scratch,
        compiler_params=pltpu.CompilerParams(collective_id=0, has_side_effects=True, vmem_limit_bytes=38 * 2**20),
        cost_estimate=pl.CostEstimate(flops=6 * 2 * 2048 * 640 * 2560, bytes_accessed=100 * 2**20, transcendentals=0),
    )(*parts, *blocks, *moments)


def put_kernel(*refs):
    n = len(refs) // 2
    copies = [pltpu.make_async_copy(src, dst, refs[-1].at[i]) for i, (src, dst) in enumerate(zip(refs[:n], refs[n : 2 * n]))]
    for c in copies:
        c.start()
    for c in copies:
        c.wait()


def put(arrays):
    return pl.pallas_call(
        put_kernel,
        in_specs=[pl.BlockSpec(memory_space=pltpu.VMEM)] * len(arrays),
        out_specs=[pl.BlockSpec(memory_space=pltpu.HBM)] * len(arrays),
        out_shape=[jax.ShapeDtypeStruct(a.shape, a.dtype) for a in arrays],
        scratch_shapes=[pltpu.SemaphoreType.DMA((len(arrays),))],
        compiler_params=pltpu.CompilerParams(vmem_limit_bytes=2**20),
    )(*arrays)


def solution(mesh):
    def step(x, dy, wg, wu, wd, *moments):
        parts = chain(x[0], dy[0], wg, wu, wd)
        new = put(comm(parts, (wg, wu, wd), moments))
        return tuple(t.reshape(w.shape) for t, w in zip(new, (wg, wu, wd))) + tuple(new[3:])

    whole, rows = P(None, None, None), P(None, "dp", None)
    return jax.shard_map(
        step,
        mesh=mesh,
        in_specs=(P(("rep", "dp")),) * 2 + (whole,) * 3 + (rows,) * 6,
        out_specs=(P("rep", None, None),) * 3 + (P("rep", "dp", None),) * 6,
        check_vma=False,
    )
```

```python
import jax
import jax.numpy as jnp
from jax import lax
from jax.experimental import pallas as pl
from jax.experimental.pallas import tpu as pltpu
from jax.sharding import PartitionSpec as P

F32, BF16 = jnp.float32, jnp.bfloat16
NT = (((1,), (1,)), ((), ()))


def dot(a, b):
    return jnp.dot(a, b, preferred_element_type=F32)


def dot_t(a, b):
    return lax.dot_general(a, b, NT, preferred_element_type=F32)


def sigmoid(x):
    return 0.5 * jnp.tanh(0.5 * x) + 0.5


def norm_scale(h):
    wide = h.astype(F32)
    return wide, lax.rsqrt(jnp.mean(wide * wide, -1, keepdims=True) + 1e-6)


def chain_kernel(x_ref, dy_ref, wg_hbm, wu_hbm, wd_hbm, act2_ref, dg2_ref, du2_ref, act1_ref, dg1_ref, du1_ref, at1_ref, at2_ref, dyt_ref, dht_ref,
                 wg, wu, wd, gate1, up1, sems, *, ft):
    ff = wg.shape[2]
    i = pl.program_id(0)
    copies = [pltpu.make_async_copy(src.at[l], dst.at[l], sems.at[l, k]) for l in range(2) for k, (src, dst) in enumerate(((wg_hbm, wg), (wu_hbm, wu), (wd_hbm, wd)))]

    def ask(*which):
        @pl.when(i == 0)
        def _():
            for n in which:
                copies[n].start()

    ask(0, 1)

    def arrived(n):
        @pl.when(i == 0)
        def _():
            copies[n].wait()

    x = x_ref[...]
    dy = dy_ref[...]
    wide, s = norm_scale(x)
    a = (wide * s).astype(BF16)
    at1_ref[...] = a.T
    dyt_ref[...] = dy.T
    arrived(0)
    arrived(1)
    ask(2)
    total = jnp.zeros(x.shape, F32)
    for f in range(0, ff, ft):
        fs = pl.ds(f, ft)
        gate = dot(a, wg[0, :, fs])
        up = dot(a, wu[0, :, fs])
        gate1[:, fs] = gate
        up1[:, fs] = up
        act = (gate * sigmoid(gate) * up).astype(BF16)
        act1_ref[:, fs] = act
        if f == 0:
            arrived(2)
            ask(3, 4, 5)
        total += dot(act, wd[0, fs, :])
    h = x + total.astype(BF16)
    arrived(3)
    arrived(4)
    arrived(5)
    wide, s = norm_scale(h)
    a = (wide * s).astype(BF16)
    at2_ref[...] = a.T
    dag = jnp.zeros(x.shape, F32)
    dau = jnp.zeros(x.shape, F32)

    def back(dout, gate, up, l, fs, refs):
        dact = dot_t(dout, wd[l, fs, :]).astype(BF16).astype(F32)
        sig = sigmoid(gate)
        silu = gate * sig
        du = (dact * silu).astype(BF16)
        dg = (dact * up * (sig + silu * (1.0 - sig))).astype(BF16)
        refs[0][:, fs] = dg
        refs[1][:, fs] = du
        return dg, du, silu

    for f in range(0, ff, ft):
        fs = pl.ds(f, ft)
        gate = dot(a, wg[1, :, fs])
        up = dot(a, wu[1, :, fs])
        dg, du, silu = back(dy, gate, up, 1, fs, (dg2_ref, du2_ref))
        act2_ref[:, fs] = (silu * up).astype(BF16)
        dag += dot_t(dg, wg[1, :, fs])
        dau += dot_t(du, wu[1, :, fs])
    da = (dag.astype(BF16) + dau.astype(BF16)).astype(F32)
    inner = jnp.mean(da * wide, -1, keepdims=True)
    dh = dy + (da * s - wide * (s * s * s * inner)).astype(BF16)
    dht_ref[...] = dh.T
    for f in range(0, ff, ft):
        fs = pl.ds(f, ft)
        back(dh, gate1[:, fs], up1[:, fs], 0, fs, (dg1_ref, du1_ref))


def chain(x, dy, wg, wu, wd, tile=256, ft=1280):
    tokens, d = x.shape
    ff = wg.shape[2]
    rows = pl.BlockSpec((tile, d), lambda i: (i, 0))
    cols = pl.BlockSpec((d, tile), lambda i: (0, i))
    wide = pl.BlockSpec((tile, ff), lambda i: (i, 0))
    hbm = pl.BlockSpec(memory_space=pl.ANY)
    return pl.pallas_call(
        lambda *r: chain_kernel(*r, ft=ft),
        grid=(tokens // tile,),
        in_specs=[rows, rows, hbm, hbm, hbm],
        out_specs=[wide] * 6 + [cols] * 4,
        out_shape=[jax.ShapeDtypeStruct((tokens, ff), BF16)] * 6 + [jax.ShapeDtypeStruct((d, tokens), BF16)] * 4,
        scratch_shapes=[pltpu.VMEM(wg.shape, BF16), pltpu.VMEM(wu.shape, BF16), pltpu.VMEM(wd.shape, BF16), pltpu.VMEM((tile, ff), F32), pltpu.VMEM((tile, ff), F32), pltpu.SemaphoreType.DMA((2, 3))],
        compiler_params=pltpu.CompilerParams(dimension_semantics=("arbitrary",), vmem_limit_bytes=63 * 2**20),
        cost_estimate=pl.CostEstimate(flops=9 * 2 * tokens * d * ff, bytes_accessed=100 * 2**20, transcendentals=0),
    )(x, dy, wg, wu, wd)
MESH = pl.DeviceIdType.MESH
CHUNKS = (("gate", 1), ("up", 1), ("down", 1), ("gate", 0), ("up", 0), ("down", 0))
FT = 512
SPLIT = (2, 1, 1, 1, 1, 2)
PERIOD, STEP, TILE = 13.0, 4.0, 1.7


def adamw(w, m, v, g):
    m = 0.9 * m + 0.1 * g
    v = 0.95 * v + 0.05 * g * g
    step = m * lax.rsqrt(v + 1e-8) + 0.1 * w
    return (w - 0.02 * step).astype(BF16), m, v


class Chunk:
    def __init__(self, place, bufs, own, ssem, rsem, free):
        self.__dict__.update(place)
        (self.T, self.D, self.YA, self.EA, self.FA, self.EB, self.FB, self.YB) = bufs
        self.w, self.m, self.v = own
        self.ssem, self.rsem, self.free = ssem, rsem, free
        self.R = self.T.shape[3]
        self.RA = self.R * 3 // 5
        self.A, self.B = pl.ds(0, self.RA), pl.ds(self.RA, self.R - self.RA)
        self.sent = []

    def copy(self, src, dst, s, r, dev):
        return pltpu.make_async_remote_copy(src_ref=src, dst_ref=dst, send_sem=self.ssem.at[s], recv_sem=self.rsem.at[r], device_id=dev, device_id_type=MESH)

    def send(self, cond, src, dst, s, r, dev):
        base, o = s if isinstance(s, tuple) else (s, None)
        self.copy(src, dst, base if o is None else base + o, r, dev).start()
        self.sent.append((cond, src.shape, base, o))

    def wait_sent(self):
        R, RA = self.R, self.RA
        like = {
            (2, 4, R): lambda: self.D,
            (RA,): lambda: self.YA.at[0],
            (R - RA,): lambda: self.YB,
            (2, R - RA): lambda: self.EB.at[0],
        }
        for cond, shape, base, o in self.sent[1:]:
            def wait():
                ref = like[tuple(shape[:-1])]()
                self.copy(ref, ref, base if o is None else base + o, 0, self.partner).wait_send()

            self.when(cond, wait)

    def got(self, dst, r):
        self.copy(dst, dst, 0, r, self.partner).wait_recv()

    def when(self, cond, f):
        if cond is None:
            f()
        else:
            pl.when(cond)(f)

    def add(self, dst, *srcs):
        dst[...] = sum(s[...].astype(F32) for s in (dst, *srcs)).astype(BF16)

    def own_y(self, o, rows):
        return self.T.at[self.y, o, self.c, rows, :]

    def both(self, o):
        return self.T.at[:, o, self.c, self.B, :]

    def s0(self):
        self.send(None, self.T.at[:, :, 1 - self.c], self.D, 0, 0, self.partner)

    def s1(self):
        self.got(self.D, 0)
        for n, o in enumerate((self.e1, self.i1, self.i0, self.e0)):
            t = self.D.at[1 - self.y, o, self.A, :]
            self.add(t, self.T.at[1 - self.y, o, self.c, self.A, :])
            self.send(None, t, self.YA.at[o], (1, o), 1 + o, self.across)

        def end():
            for slot, o in enumerate((self.e1, self.i1, self.i0)):
                t = self.D.at[:, o, self.B, :]
                self.add(t, self.both(o))
                self.send(self.end, t, self.EB.at[slot], 11 + slot, 11 + slot, self.inner)

        self.when(self.end, end)

    def s2(self):
        self.copy(self.D, self.D, 0, 0, self.partner).wait_send()
        pl.semaphore_signal(self.free, inc=1, device_id=self.partner, device_id_type=MESH)

        def mid():
            for slot, o in enumerate((self.e1, self.i1)):
                self.got(self.EB.at[slot], 11 + slot)
                t = self.D.at[:, o, self.B, :]
                self.add(t, self.both(o), self.EB.at[slot])
                self.send(self.mid, t, self.FB.at[slot], 14 + slot, 14 + slot, self.inner)

        self.when(self.mid, mid)

    def got_y(self, o):
        self.got(self.YA.at[o], 1 + o)

    def s3(self):
        def end():
            for slot, o in enumerate((self.e1, self.i1, self.i0)):
                self.got_y(o)
                t = self.YA.at[o]
                self.add(t, self.own_y(o, self.A), self.D.at[self.y, o, self.A, :])
                self.send(self.end, t, self.EA.at[slot], 5 + slot, 5 + slot, self.inner)

        def mid():
            self.got(self.FB.at[0], 14)
            t = self.D.at[:, self.e0, self.B, :]
            self.add(t, self.both(self.e0), self.FB.at[0])
            self.send(self.mid, t, self.FB.at[1], 16, 16, self.outer)

        self.when(self.end, end)
        self.when(self.mid, mid)

    def s4(self):
        def mid():
            for slot, o in enumerate((self.e1, self.i1)):
                self.got(self.EA.at[slot], 5 + slot)
                self.got_y(o)
                t = self.YA.at[o]
                self.add(t, self.own_y(o, self.A), self.D.at[self.y, o, self.A, :], self.EA.at[slot])
                self.send(self.mid, t, self.FA.at[slot], 8 + slot, 8 + slot, self.inner)

        self.when(self.mid, mid)
        own = self.T.at[1 - self.y, self.z, self.c, self.B, :]
        d = self.D.at[1 - self.y, self.z, self.B, :]
        t = self.FB.at[1, 1 - self.y]

        def mid2():
            self.got(self.FB.at[1], 15)
            self.got(self.EB.at[2], 13)
            self.add(t, own, d, self.EB.at[2, 1 - self.y])

        def end2():
            self.got(self.FB.at[1], 16)
            self.add(t, own, d)

        self.when(self.mid, mid2)
        self.when(self.end, end2)
        self.send(None, t, self.YB, 17, 17, self.across)

    def step(self, rows, *srcs):
        t = self.own_y(self.z, rows)
        g = sum(s[...].astype(F32) for s in (t, *srcs)).astype(BF16).astype(F32)
        w, m, v = adamw(self.w[rows, :].astype(F32), self.m[rows, :], self.v[rows, :], g)
        t[...] = w
        self.m[rows, :] = m
        self.v[rows, :] = v

    def s5(self):
        def mid():
            self.got(self.FA.at[0], 8)
            self.got_y(self.e0)
            t = self.YA.at[self.e0]
            self.add(t, self.own_y(self.e0, self.A), self.D.at[self.y, self.e0, self.A, :], self.FA.at[0])
            self.send(self.mid, t, self.FA.at[1], 10, 10, self.outer)

        self.when(self.mid, mid)
        self.got(self.YB, 17)
        d = self.D.at[self.y, self.z, self.B, :]
        self.when(self.mid, lambda: self.step(self.B, d, self.YB, self.FB.at[1, self.y], self.EB.at[2, self.y]))
        self.when(self.end, lambda: self.step(self.B, d, self.YB, self.FB.at[1, self.y]))
        t = self.own_y(self.z, self.B)
        self.send(None, t, t, 30, 30, self.across)

    def s6(self):
        self.got_y(self.z)
        d = self.D.at[self.y, self.z, self.A, :]

        def mid():
            self.got(self.FA.at[1], 9)
            self.got(self.EA.at[2], 7)
            self.step(self.A, d, self.YA.at[self.z], self.FA.at[1], self.EA.at[2])

        def end():
            self.got(self.FA.at[1], 10)
            self.step(self.A, d, self.YA.at[self.z], self.FA.at[1])

        self.when(self.mid, mid)
        self.when(self.end, end)
        self.give_a(self.z, None, self.mid, None)
        self.got(self.T.at[1 - self.y, self.z, self.c, self.B, :], 30)
        self.give_b(self.z, None, self.mid)

    def give_a(self, o, inward, outward, cond):
        t = self.own_y(o, self.A)
        if inward is not False:
            self.when(inward, lambda: self.send(inward, t, t, (18, o), 18 + o, self.inner))
        if outward is not False:
            self.when(outward, lambda: self.send(outward, t, t, (22, o), 18 + o, self.outer))
        self.send(cond, t, t, (26, o), 26 + o, self.across)

    def give_b(self, o, inward, outward):
        t = self.both(o)
        if inward is not False:
            self.when(inward, lambda: self.send(inward, t, t, (31, o), 31 + o, self.inner))
        if outward is not False:
            self.when(outward, lambda: self.send(outward, t, t, (35, o), 31 + o, self.outer))

    def got_a(self, o):
        self.got(self.own_y(o, self.A), 18 + o)

    def got_b(self, o):
        self.got(self.both(o), 31 + o)

    def plain(self, cond, o, inward, outward, which):
        if which == "a":
            t = self.own_y(o, self.A)
            self.got_a(o)
            base = 18
        else:
            t = self.both(o)
            self.got_b(o)
            base = 31
        if inward:
            self.send(cond, t, t, (base, o), base + o, self.inner)
        if outward:
            self.send(cond, t, t, (base + 4, o), base + o, self.outer)
        if which == "a":
            self.send(cond, t, t, (26, o), 26 + o, self.across)

    def g1(self, which):
        def mid():
            self.plain(self.mid, self.e0, True, False, which)
            self.plain(self.mid, self.i1, False, True, which)

        self.when(self.mid, mid)
        self.when(self.end, lambda: self.plain(self.end, self.i0, False, False, which))

    def g2(self, which):
        self.when(self.mid, lambda: self.plain(self.mid, self.e1, False, True, which))
        self.when(self.end, lambda: self.plain(self.end, self.i1, False, False, which))

    def g3(self, which):
        self.when(self.end, lambda: self.plain(self.end, self.e1, False, False, which))

    def s7(self):
        self.g1("a")

    def s8(self):
        self.g1("b")
        self.g2("a")

    def s9(self):
        self.g2("b")
        self.g3("a")

    def s10(self):
        self.g3("b")
        for o in range(4):
            self.got(self.T.at[1 - self.y, o, self.c, self.A, :], 26 + o)
        pl.semaphore_wait(self.free, 1)
        t = self.T.at[:, :, self.c]
        self.send(None, t, t, 39, 39, self.partner)

    def s11(self):
        self.got(self.T.at[:, :, 1 - self.c], 39)
        self.wait_sent()

    STEPS = ("s0", "s1", "s2", "s3", "s4", "s5", "s6", "s7", "s8", "s9", "s10", "s11")


def kernel(act2, dg2, du2, act1, dg1, du1, at1, at2, dyt, dht, wg, wu, wd, mg, mu, md, vg, vu, vd,
           tg, tu, td, sm_g, sm_u, sm_d, sv_g, sv_u, sv_d,
           dG, dDn, yaG, yaD, eaG, eaD, faG, faD, ebG, ebD, fbG, fbD, ybG, ybD,
           lhs, rhs, sw_g, sw_u, sw_d,
           ssem, rsem, lsem, tsem, isem, free):
    rep, me = lax.axis_index("rep"), lax.axis_index("dp")
    c, z, y = me % 2, (me // 2) % 4, me // 8

    def dev(y, z, c):
        return (rep, y * 8 + z * 2 + c)

    low = z < 2
    e0, i0, i1, e1 = (jnp.where(low, p, 3 - p) for p in range(4))
    end = (z == 0) | (z == 3)
    mid = (z == 1) | (z == 2)
    inner = dev(y, jnp.where(end, i0, i1), c)
    outer = dev(y, e0, c)
    place = dict(y=y, z=z, c=c, e0=e0, i0=i0, i1=i1, e1=e1, end=end, mid=mid, inner=inner, outer=outer, across=dev(1 - y, z, c), partner=dev(y, z, 1 - c))

    owns = {"gate": (sw_g, sm_g, sv_g), "up": (sw_u, sm_u, sv_u), "down": (sw_d, sm_d, sv_d)}
    T = {"gate": tg, "up": tu, "down": td}
    loads = []
    for n, (name, hw, hm, hv) in enumerate((("gate", wg, mg, vg), ("up", wu, mu, vu), ("down", wd, md, vd))):
        sw, sm, sv = owns[name]
        loads += [pltpu.make_async_copy(hw.at[:, me], sw, isem.at[n, 0]), pltpu.make_async_copy(hm, sm, isem.at[n, 1]), pltpu.make_async_copy(hv, sv, isem.at[n, 2])]

    left = {("down", 1): dyt, ("gate", 1): at2, ("up", 1): at2, ("down", 0): dht, ("gate", 0): at1, ("up", 0): at1}
    right = {("down", 1): act2, ("gate", 1): dg2, ("up", 1): du2, ("down", 0): act1, ("gate", 0): dg1, ("up", 0): du1}
    tiles = right[CHUNKS[0]].shape[1] // FT

    def rhs_copy(k, j):
        t = tiles * k + j
        return pltpu.make_async_copy(right[CHUNKS[k]].at[:, pl.ds(j * FT, FT)], rhs.at[t % 2], tsem.at[t % 2])

    def lhs_copy(k):
        s = 0 if CHUNKS[k][0] == "down" else 1
        return pltpu.make_async_copy(left[CHUNKS[k]], lhs.at[s], lsem.at[s])

    lhs_copy(0).start()
    rhs_copy(0, 0).start()
    lhs_copy(2).start()

    barrier = pltpu.get_barrier_semaphore()
    for d, cond in ((place["partner"], None), (place["across"], None), (inner, None), (outer, mid)):
        if cond is None:
            pl.semaphore_signal(barrier, inc=1, device_id=d, device_id_type=MESH)
        else:
            @pl.when(cond)
            def _():
                pl.semaphore_signal(barrier, inc=1, device_id=d, device_id_type=MESH)
    pl.when(mid)(lambda: pl.semaphore_wait(barrier, 4))
    pl.when(end)(lambda: pl.semaphore_wait(barrier, 3))

    def part(k, ref, h):
        if SPLIT[k] == 1:
            return ref
        rows, cols = ref.shape[-2] // SPLIT[k], ref.shape[-1] // SPLIT[k]
        lead = (slice(None),) * (len(ref.shape) - 2)
        if CHUNKS[k][0] == "down":
            return ref.at[lead + (pl.ds(h * rows, rows), slice(None))]
        return ref.at[lead + (slice(None), pl.ds(h * cols, cols))]

    chunks, which = [], []
    counts = [0, 0]
    for k, (name, l) in enumerate(CHUNKS):
        pick = 1 if name == "down" else 0
        n = counts[pick]
        counts[pick] += 1
        for h in range(SPLIT[k]):
            bufs = [T[name].at[l]] + [b[pick].at[n] for b in ((dG, dDn), (yaG, yaD), (eaG, eaD), (faG, faD), (ebG, ebD), (fbG, fbD), (ybG, ybD))]
            i = len(chunks)
            chunks.append(Chunk(place, [part(k, b, h) for b in bufs], [part(k, b.at[l], h) for b in owns[name]], ssem.at[i], rsem.at[i], free.at[i]))
            which.append((k, h))

    def run(k, s):
        if (k, s) == (0, 5):
            for cp in loads:
                cp.wait()
        getattr(chunks[k], Chunk.STEPS[s])()

    def ready(i):
        k, h = which[i]
        return tiles * (k + 1) - 1 if CHUNKS[k][0] == "down" else tiles * k - (-tiles * (h + 1) // SPLIT[k]) - 1

    plan = sorted((max(ready(i), ready(0) + (PERIOD * (which[i][0] + which[i][1] / SPLIT[which[i][0]]) + STEP * s) / TILE) + s * 1e-6, i, s) for i in range(len(chunks)) for s in range(len(Chunk.STEPS)))
    total_tiles = tiles * len(CHUNKS)
    slots = {}
    for at, k, s in plan:
        slots.setdefault(min(int(at), total_tiles), []).append((k, s))

    for k, (name, l) in enumerate(CHUNKS):
        if k == 0:
            for cp in loads:
                cp.start()
        if k in (0, 2, 3, 5):
            lhs_copy(k).wait()
        side = 0 if name == "down" else 1

        def tile(j, _, k=k, name=name, l=l, side=side):
            t = tiles * k + j
            rhs_copy(k, j).wait()

            @pl.when(j < tiles - 1)
            def _():
                rhs_copy(k, j + 1).start()

            if k + 1 < len(CHUNKS):
                @pl.when(j == tiles - 1)
                def _():
                    rhs_copy(k + 1, 0).start()

            out = jnp.dot(lhs[side], rhs[t % 2], preferred_element_type=F32).astype(BF16)
            if name == "down":
                out = out.T
                for q in range(FT // 32):
                    n = (FT // 32) * j + q
                    b, r = n // 5, pl.multiple_of((n % 5) * 32, 32)
                    td[l, b // 8, (b // 2) % 4, b % 2, pl.ds(r, 32), :] = out[32 * q : 32 * q + 32]
            else:
                T[name][l, :, :, :, :, pl.ds(pl.multiple_of(j * FT, FT), FT)] = out.reshape(2, 4, 2, 40, FT)
            for jj in range(tiles):
                todo = slots.get(tiles * k + jj, [])
                if todo:
                    @pl.when(j == jj)
                    def _(todo=todo):
                        for kk, s in todo:
                            run(kk, s)
            return 0

        lax.fori_loop(0, tiles, tile, 0)
        if k in (1, 2):
            lhs_copy(2 * k + 1).start()
    for kk, s in slots.get(total_tiles, []):
        run(kk, s)


def comm(parts, weights, moments, ):
    hbm = pl.BlockSpec(memory_space=pl.ANY)
    wg, wu, wd = weights
    blocks = [w.reshape(w.shape[0], 16, w.shape[1] // 16, w.shape[2]) for w in weights]
    outs = [pltpu.VMEM((2, 2, 4, 2) + b.shape[2:], BF16) for b in blocks]
    outs += [pltpu.VMEM(t.shape, F32) for t in moments]
    g, d = (40, 2560), (160, 640)

    def pair(*lead, a=None):
        def rows(s):
            return {None: s[0], "A": s[0] * 3 // 5, "B": s[0] * 2 // 5}[a]
        return [pltpu.VMEM((4, *lead, rows(g), g[1]), BF16), pltpu.VMEM((2, *lead, rows(d), d[1]), BF16)]

    scratch = pair(2, 4) + pair(4, a="A") + pair(3, a="A") + pair(2, a="A") + pair(3, 2, a="B") + pair(2, 2, a="B") + pair(a="B")
    scratch += [pltpu.VMEM((2, 640, 2048), BF16), pltpu.VMEM((2, 2048, FT), BF16)]
    scratch += [pltpu.VMEM((2,) + b.shape[2:], BF16) for b in blocks]
    dma = pltpu.SemaphoreType.DMA
    scratch += [dma((sum(SPLIT), 40)), dma((sum(SPLIT), 40)), dma((2,)), dma((2,)), dma((3, 3)), pltpu.SemaphoreType.REGULAR((sum(SPLIT),))]
    return pl.pallas_call(
        kernel,
        in_specs=[hbm] * 19,
        out_specs=[pl.BlockSpec(memory_space=pltpu.VMEM)] * 9,
        out_shape=outs,
        scratch_shapes=scratch,
        compiler_params=pltpu.CompilerParams(collective_id=0, has_side_effects=True, vmem_limit_bytes=38 * 2**20),
        cost_estimate=pl.CostEstimate(flops=6 * 2 * 2048 * 640 * 2560, bytes_accessed=100 * 2**20, transcendentals=0),
    )(*parts, *blocks, *moments)


def put_kernel(*refs):
    n = len(refs) // 2
    copies = [pltpu.make_async_copy(src, dst, refs[-1].at[i]) for i, (src, dst) in enumerate(zip(refs[:n], refs[n : 2 * n]))]
    for c in copies:
        c.start()
    for c in copies:
        c.wait()


def put(arrays):
    return pl.pallas_call(
        put_kernel,
        in_specs=[pl.BlockSpec(memory_space=pltpu.VMEM)] * len(arrays),
        out_specs=[pl.BlockSpec(memory_space=pltpu.HBM)] * len(arrays),
        out_shape=[jax.ShapeDtypeStruct(a.shape, a.dtype) for a in arrays],
        scratch_shapes=[pltpu.SemaphoreType.DMA((len(arrays),))],
        compiler_params=pltpu.CompilerParams(vmem_limit_bytes=2**20),
    )(*arrays)


def solution(mesh):
    def step(x, dy, wg, wu, wd, *moments):
        parts = chain(x[0], dy[0], wg, wu, wd)
        new = put(comm(parts, (wg, wu, wd), moments))
        return tuple(t.reshape(w.shape) for t, w in zip(new, (wg, wu, wd))) + tuple(new[3:])

    whole, rows = P(None, None, None), P(None, "dp", None)
    return jax.shard_map(
        step,
        mesh=mesh,
        in_specs=(P(("rep", "dp")),) * 2 + (whole,) * 3 + (rows,) * 6,
        out_specs=(P("rep", None, None),) * 3 + (P("rep", "dp", None),) * 6,
        check_vma=False,
    )
```
